256 devices in a mesh: dp: 64 (over z, x, core), psr: 4 (over y).
Axes of the slice: x: 4, y: 4, z: 8, core: 2. Of those that a mesh axis runs over, the one named last changes fastest.
Arguments:
- basis: bfloat16 [256, 4, 8, 128, 256], P(('dp', 'psr')), may hold values from -6 to 6
- residual: bfloat16 [256, 4, 8, 128], P(('dp', 'psr')), may hold values from -6 to 6
- sigma: bfloat16 [256, 4, 8, 128], P(('dp', 'psr')), may hold values from 0.5 to 2
- counts: int32 [256, 4, 8], P(('dp', 'psr')), may hold values from 0 to 128
- pulsar: int32 [256, 4, 8], P(('dp', 'psr')), may hold values from 0 to 3
- ecorr: float32 [16], replicated, may hold values from 0.2 to 2
Outputs:
- gram: float32 [16, 256, 256], P('psr', 'dp')
- rhs: float32 [16, 256], P('psr', 'dp')
- totals: float32 [2], replicated
The draws below stay inside these ranges and needn't reach their ends.
All inputs are finite; a program needn't handle non-finite values.
Results may differ from the reference program's by a relative error of at most 0.0055.
Values may be sent and summed in bfloat16 or wider, within the bound.
No kernel may reach another device: no remote copies, remote signals or barrier semaphores. Data moves between devices by JAX's collectives and lax.ppermute only.
A program may use at most 64 MiB of HBM per device.

```python
import math
import jax
import jax.numpy as jnp
from jax import lax

K = 256
L = 128
PG = 4
E_GRP = 8
P_SIZE = 16
SOURCES = 256
NORM_ROWS = 65536
ALL_ROWS = 1048576
N_PSR = 4


def plant(entries, stream_key, smallest, top_value):
    index_at = [jax.random.randint(jax.random.fold_in(stream_key, axis), (), 0, length) for axis, length in enumerate(entries.shape)]
    widest = entries.shape.index(max(entries.shape))
    next_to = index_at[:widest] + [(index_at[widest] + 1) % entries.shape[widest]] + index_at[widest + 1:]
    return entries.at[tuple(index_at)].set(smallest).at[tuple(next_to)].set(top_value)


def shard_levels(rng, dims, split, smallest, high):
    def one(axis_at, blocks):
        heights = jax.random.uniform(jax.random.fold_in(jax.random.fold_in(rng, 6), axis_at), (blocks,), jnp.float32, smallest / len(split), high / len(split))
        return jnp.repeat(jnp.exp(heights), dims[axis_at] // blocks).reshape((-1,) + (1,) * (len(dims) - axis_at - 1))

    loudness = one(*split[0])
    for cut in split[1:]:
        loudness = loudness * one(*cut)
    return loudness


def scatter_about(rng, shape, width, reach, shards=(), kind=jnp.bfloat16):
    gain = shard_levels(rng, shape, shards, -0.22, 0.18) if shards else 1.0
    values = jax.random.normal(rng, shape, jnp.float32) * width * gain
    return jnp.minimum(jnp.maximum(values, -reach), reach).astype(kind)


def setup_inputs(seed: int = 0) -> dict:
    seeds = jax.random.split(jax.random.key(seed), 7)
    basis = scatter_about(seeds[0], (SOURCES, N_PSR, E_GRP, L, K), 1.0, 6.0, ((0, 256),))
    residual = scatter_about(seeds[1], (SOURCES, N_PSR, E_GRP, L), 1.0, 6.0, ((0, 256),))
    sigma = jnp.clip(jnp.exp(math.log(2.0) - 1.3862944 * jax.random.uniform(seeds[2], (SOURCES, N_PSR, E_GRP, L), jnp.float32) ** shard_levels(seeds[2], (SOURCES, N_PSR, E_GRP, L), ((0, 256),), -0.2, 0.2)), 0.5, 2.0).astype(jnp.bfloat16)
    counts = plant(jax.random.randint(seeds[3], (SOURCES, N_PSR, E_GRP), 0, L + 1), jax.random.fold_in(seeds[3], 1), 0, L).astype(jnp.int32)
    pulsar = plant(jax.random.randint(seeds[4], (SOURCES, N_PSR, E_GRP), 0, PG), jax.random.fold_in(seeds[4], 1), 0, PG - 1).astype(jnp.int32)
    ecorr = jnp.clip(jnp.exp(jax.random.uniform(seeds[5], (P_SIZE,), jnp.float32, math.log(0.2), math.log(2.0))), 0.2, 2.0)
    return {"basis": basis, "residual": residual, "sigma": sigma, "counts": counts, "pulsar": pulsar, "ecorr": ecorr}


def block_terms(basis, residual, sigma, counts, pulsar, ecorr):
    sig = sigma.astype(jnp.float32)
    res = residual.astype(jnp.float32)
    rowpos = lax.broadcasted_iota(jnp.int32, sig.shape, 2)
    valid = rowpos < counts[..., None]
    inverse = jnp.where(valid, 1.0 / (sig * sig), jnp.float32(0.0))
    weighted = (inverse[..., None] * basis.astype(jnp.float32)).astype(jnp.bfloat16)
    weighted_f = weighted.astype(jnp.float32)
    groups = jnp.arange(N_PSR, dtype=jnp.int32)
    global_id = (groups[:, None] * PG + pulsar).astype(jnp.int32)
    jitter = ecorr[global_id] ** 2
    total = jnp.sum(inverse, axis=2)
    coef = jitter / (1.0 + jitter * total)
    column = jnp.sum(weighted_f, axis=2)
    project = jnp.sum(weighted_f * res[..., None], axis=2)
    wsum = jnp.sum(inverse * res, axis=2)
    chi = jnp.sum(inverse * res * res) - jnp.sum(coef * wsum * wsum)
    logdet = jnp.sum(jnp.where(valid, jnp.log(sig * sig), jnp.float32(0.0))) + jnp.sum(jnp.log(1.0 + jitter * total))
    first = jnp.einsum('gslk,gslm->gskm', basis.astype(jnp.float32), weighted_f, precision=lax.Precision.HIGHEST)
    onehot = (pulsar[..., None] == jnp.arange(PG, dtype=jnp.int32)).astype(jnp.float32)
    gram = jnp.einsum('gsp,gskm->gpkm', onehot, first, precision=lax.Precision.HIGHEST)
    gram = gram - jnp.einsum('gsp,gsk,gsm->gpkm', onehot * coef[..., None], column, column, precision=lax.Precision.HIGHEST)
    rhs = jnp.einsum('gsp,gsk->gpk', onehot, project - (coef * wsum)[..., None] * column, precision=lax.Precision.HIGHEST)
    return gram, rhs, logdet, chi


def reference(basis, residual, sigma, counts, pulsar, ecorr):
    def step(carry, items):
        gram, rhs, logdet, chi = block_terms(items[0], items[1], items[2], items[3], items[4], ecorr)
        return (carry[0] + gram, carry[1] + rhs, carry[2] + logdet, carry[3] + chi), None

    start = (jnp.zeros((N_PSR, PG, K, K), jnp.float32), jnp.zeros((N_PSR, PG, K), jnp.float32), jnp.float32(0.0), jnp.float32(0.0))
    final, _ = lax.scan(step, start, (basis, residual, sigma, counts, pulsar))
    gram = final[0].reshape(P_SIZE, K, K) / NORM_ROWS
    rhs = final[1].reshape(P_SIZE, K) / NORM_ROWS
    totals = jnp.stack([final[2], final[3]]) / ALL_ROWS
    return gram, rhs, totals
```

```python
import functools

import jax
import jax.numpy as jnp
from jax import lax
from jax.experimental import pallas as pl
from jax.experimental.pallas import tpu as pltpu
from jax.sharding import Mesh
from jax.sharding import PartitionSpec as P


PG = 4
AXES = ("z", "x", "c", "psr")
BF = jnp.bfloat16
F32 = jnp.float32
HALF = 128
DIRECT = (((0,), (0,)), ((), ()))


def split2(e):
    head = e.astype(BF).astype(F32)
    return jnp.concatenate([head, e - head], axis=0).astype(BF)


def joined2(x):
    full = x.astype(F32)
    rows = full.shape[0] // 2
    return full[:rows] + full[rows:]


def row_in(rows, width, items):
    sub = lax.broadcasted_iota(jnp.int32, (rows, width), 0)
    out = jnp.zeros((rows, width), F32)
    for at, item in items:
        out = jnp.where(sub == at, jnp.broadcast_to(item, (rows, width)), out)
    return out


def dot0(a, b):
    return lax.dot_general(a, b, DIRECT, preferred_element_type=F32)


def packed(full, rhs, totals):
    a = full[:HALF, :HALF]
    b = full[:HALF, HALF:]
    d = full[HALF:, HALF:]
    r = lax.broadcasted_iota(jnp.int32, (HALF, HALF), 0)
    c = lax.broadcasted_iota(jnp.int32, (HALF, HALF), 1)
    both = jnp.where(r >= c, a, d)
    diag = jnp.sum(jnp.where(r == c, d, 0.0), axis=0, keepdims=True)
    extras = row_in(
        8, HALF, [(0, diag), (1, rhs[:, :HALF]), (2, rhs[:, HALF:]), (3, totals)]
    )
    return b, both, extras


def terms_kernel(
    counts, pulsar, ecorr, sigma, residual, basis, keep, send, buf, sems, acc, racc, inv_s, wide_s
):
    groups, slots = counts.shape
    y = lax.axis_index("psr")
    core = lax.axis_index("c")
    copies = []
    for i in range(groups):
        g = lax.rem(y + i, groups)
        copies.append(pltpu.make_async_copy(basis.at[g], buf.at[i], sems.at[i]))
        copies[-1].start()
    lane = lax.broadcasted_iota(jnp.int32, (slots, HALF), 1)
    sub = lax.broadcasted_iota(jnp.int32, (slots, HALF), 0)
    logdet = jnp.zeros((slots, 1), F32)
    chi = jnp.zeros((slots, 1), F32)
    for g in range(groups):
        count = jnp.zeros((slots, HALF), jnp.int32)
        amp = jnp.zeros((slots, HALF), F32)
        for s in range(slots):
            count = jnp.where(sub == s, counts[g, s], count)
            amp = jnp.where(sub == s, ecorr[g * PG + pulsar[g, s]], amp)
        sig = sigma[g].astype(F32)
        res = residual[g].astype(F32)
        square = sig * sig
        valid = lane < count
        inverse = jnp.where(valid, 1.0 / square, 0.0)
        scaled = inverse * res
        total = jnp.sum(inverse, axis=1, keepdims=True)
        wsum = jnp.sum(scaled, axis=1, keepdims=True)
        jitter = amp * amp
        grown = 1.0 + jitter * total
        coef = jitter / grown
        logs = jnp.sum(jnp.where(valid, jnp.log(square), 0.0), axis=1, keepdims=True)
        logdet = logdet + logs + jnp.log(grown)[:, :1]
        chi = chi + jnp.sum(scaled * res, axis=1, keepdims=True) - coef[:, :1] * wsum * wsum
        inv_s[g, 0] = inverse
        inv_s[g, 1] = res
        wide_s[g, 0] = coef
        wide_s[g, 1] = coef * wsum
    lane1 = lax.broadcasted_iota(jnp.int32, (1, HALF), 1)
    totals = jnp.where(
        lane1 == 0,
        jnp.sum(logdet, axis=0, keepdims=True),
        jnp.where(lane1 == 1, jnp.sum(chi, axis=0, keepdims=True), 0.0),
    )
    nothing = jnp.zeros((1, HALF), F32)
    for i in range(groups):
        g = lax.rem(y + i, groups)
        acc[...] = jnp.zeros_like(acc)
        racc[...] = jnp.zeros_like(racc)
        inverse_t = jnp.transpose(inv_s[g, 0])
        res_t = jnp.transpose(inv_s[g, 1])
        coef = wide_s[g, 0]
        pull = wide_s[g, 1]
        member = jnp.zeros((slots, HALF), jnp.int32)
        columns = []
        copies[i].wait()
        for s in range(slots):
            block = buf[i, s]
            weighted = (block.astype(F32) * inverse_t[:, s : s + 1]).astype(BF)
            weighted_f = weighted.astype(F32)
            column = jnp.sum(weighted_f, axis=0, keepdims=True)
            project = jnp.sum(weighted_f * res_t[:, s : s + 1], axis=0, keepdims=True)
            mine = pulsar[g, s]
            member = jnp.where(sub == s, mine, member)
            acc[mine] += dot0(block, weighted)
            racc[mine, 0:1, :] += project - pull[s : s + 1, 0:1] * column
            columns.append((s, column))
        cols = row_in(slots, 2 * HALF, columns)
        head = cols.astype(BF).astype(F32)
        rest = cols - head
        left = jnp.concatenate([head, rest, head, rest], axis=0).astype(BF)
        for at in range(PG):
            to = (core if at < 2 else 1 - core) * 2 + at % 2
            scale = jnp.where(member == to, coef, 0.0)
            scaled = jnp.concatenate([scale, scale], axis=1) * cols
            high = scaled.astype(BF).astype(F32)
            low = scaled - high
            right = jnp.concatenate([high, high, low, low], axis=0).astype(BF)
            full = acc[to] - dot0(left, right)
            b, both, extras = packed(
                full, racc[to, 0:1, :], totals if at % 2 == 0 else nothing
            )
            if at < 2:
                keep[i, at, 0:HALF, :] = b
                keep[i, at, HALF : 2 * HALF, :] = both
                keep[i, at, 2 * HALF :, :] = extras
            else:
                send[i, at - 2, 0:HALF, :] = b.astype(BF)
                send[i, at - 2, HALF : 2 * HALF, :] = both.astype(BF)
                send[i, at - 2, 2 * HALF :, :] = split2(extras)


def local_terms(basis, residual, sigma, counts, pulsar, ecorr):
    groups, slots, rows, width = basis.shape
    smem = pl.BlockSpec(memory_space=pltpu.SMEM)
    vmem = pl.BlockSpec(memory_space=pltpu.VMEM)
    return pl.pallas_call(
        terms_kernel,
        name="terms",
        out_shape=(
            jax.ShapeDtypeStruct((groups, 2, 2 * HALF + 8, HALF), F32),
            jax.ShapeDtypeStruct((groups, 2, 2 * HALF + 16, HALF), BF),
        ),
        in_specs=[smem, smem, smem, vmem, vmem, pl.BlockSpec(memory_space=pl.ANY)],
        out_specs=(vmem, vmem),
        scratch_shapes=[
            pltpu.VMEM((groups, slots, rows, width), BF),
            pltpu.SemaphoreType.DMA((groups,)),
            pltpu.VMEM((PG, width, width), F32),
            pltpu.VMEM((PG, 8, width), F32),
            pltpu.VMEM((groups, 2, slots, rows), F32),
            pltpu.VMEM((groups, 2, slots, rows), F32),
        ],
    )(counts, pulsar, ecorr, sigma, residual, basis)


def cores_kernel(keep, got, *outs):
    for i, out in enumerate(outs):
        for j in range(2):
            body = keep[i + 1, j, : 2 * HALF] + got[i + 1, j, : 2 * HALF].astype(F32)
            out[j, : 2 * HALF] = body.astype(BF)
            out[j, 2 * HALF :] = split2(
                keep[i + 1, j, 2 * HALF :] + joined2(got[i + 1, j, 2 * HALF :])
            )


def unpack_kernel(keep, got, *refs):
    n = 3
    arrived, (own, *outs), full = refs[:n], refs[n:-1], refs[-1]
    x = lax.axis_index("x")
    core = lax.axis_index("c")
    r = lax.broadcasted_iota(jnp.int32, (HALF, HALF), 0)
    c = lax.broadcasted_iota(jnp.int32, (HALF, HALF), 1)
    lines = []
    for j in range(2):
        body = keep[0, j, : 2 * HALF] + got[0, j, : 2 * HALF].astype(F32)
        extras = keep[0, j, 2 * HALF :] + joined2(got[0, j, 2 * HALF :])
        for a in arrived:
            body = body + a[j, : 2 * HALF].astype(F32)
            extras = extras + joined2(a[j, 2 * HALF :])
        b, both = body[:HALF], body[HALF:]
        flipped = jnp.transpose(both)
        full[j, :HALF, :HALF] = jnp.where(r >= c, both, flipped)
        full[j, :HALF, HALF:] = b
        full[j, HALF:, :HALF] = jnp.transpose(b)
        full[j, HALF:, HALF:] = jnp.where(
            r < c, both, jnp.where(r > c, flipped, jnp.broadcast_to(extras[0:1], (HALF, HALF)))
        )
        lines.append((j, jnp.concatenate([extras[1:2], extras[2:3]], axis=1)))
        if j == 0:
            totals = jnp.concatenate([extras[3:4], jnp.zeros((1, HALF), F32)], axis=1)
    extras = row_in(8, 2 * HALF, lines + [(4, totals)])
    coded = split2(extras)
    sub = lax.broadcasted_iota(jnp.int32, (8, 2 * HALF), 0)
    for sx in range(4):
        to = lax.rem(x + sx, 4)
        tiles = [[], []]
        for z in range(8):
            at = pl.ds(pl.multiple_of(32 * z + 8 * to, 8), 8)
            t0, t1 = full[0, at, :], full[1, at, :]
            first = jnp.where(sub < 4, t0, jnp.roll(t1, 4, axis=0))
            second = jnp.where(sub < 4, jnp.roll(t0, 4, axis=0), t1)
            tiles[0].append(jnp.where(core == 0, first, second))
            tiles[1].append(jnp.where(core == 0, second, first))
        for sc in range(2):
            block = jnp.concatenate(tiles[sc], axis=0)
            if sx == 0 and sc == 0:
                own[:64] = block
                own[64:] = extras
            else:
                out = outs[2 * sx + sc - 1]
                out[:64] = block.astype(BF)
                out[64:] = coded


def columns_kernel(own, *refs):
    arrived, (kept, *outs), rows = refs[:7], refs[7:-1], refs[-1]
    z = lax.axis_index("z")
    core = lax.axis_index("c")
    same = own[:64]
    same_e = own[64:]
    other = jnp.zeros_like(same)
    other_e = jnp.zeros_like(same_e)
    for k, a in enumerate(arrived):
        if (k + 1) % 2 == 0:
            same = same + a[:64].astype(F32)
            same_e = same_e + joined2(a[64:])
        else:
            other = other + a[:64].astype(F32)
            other_e = other_e + joined2(a[64:])
    rows[0] = jnp.where(core == 0, same, other)
    rows[1] = jnp.where(core == 0, other, same)
    sub = lax.broadcasted_iota(jnp.int32, (8, 2 * HALF), 0)
    first = jnp.where(core == 0, same_e, other_e)
    second = jnp.where(core == 0, other_e, same_e)
    extras = jnp.where(
        sub < 2, first, jnp.where(sub < 4, jnp.roll(second, 2, axis=0), same_e)
    )
    coded = split2(extras)
    for sz in range(8):
        to = lax.rem(z + sz, 8)
        at = pl.ds(pl.multiple_of(8 * to, 8), 8)
        block = jnp.concatenate([rows[0, at, :], rows[1, at, :]], axis=0)
        if sz == 0:
            kept[:16] = block
            kept[16:] = extras
        else:
            outs[sz - 1][:16] = block.astype(BF)
            outs[sz - 1][16:] = coded


def final_kernel(norm, every, kept, *refs):
    arrived, (gram, rhs, totals) = refs[:7], refs[7:]
    at = 8 * lax.axis_index("z") + 2 * lax.axis_index("x") + lax.axis_index("c")
    block = kept[:16]
    extras = kept[16:]
    for a in arrived:
        block = block + a[:16].astype(F32)
        extras = extras + joined2(a[16:])
    block = block * (1.0 / norm)
    for q in range(4):
        gram[q] = block[4 * q : 4 * q + 4]
    lane = lax.broadcasted_iota(jnp.int32, (8, 2 * HALF), 1)
    lane4 = lax.broadcasted_iota(jnp.int32, (8, 4), 1)
    picked = jnp.zeros((8, 4), F32)
    for k in range(4):
        one = jnp.sum(jnp.where(lane == 4 * at + k, extras, 0.0), axis=1, keepdims=True)
        picked = jnp.where(lane4 == k, one, picked)
    rhs[...] = picked[:4] * (1.0 / norm)
    sub = lax.broadcasted_iota(jnp.int32, (8, 2 * HALF), 0)
    for k in range(2):
        totals[k] = jnp.sum(jnp.where((sub == 4) & (lane == k), extras, 0.0)) * (1.0 / every)


def call(kernel, name, outs, scratch, operands, out_specs=None):
    vmem = pl.BlockSpec(memory_space=pltpu.VMEM)
    return pl.pallas_call(
        kernel,
        name=name,
        out_shape=tuple(jax.ShapeDtypeStruct(s, d) for s, d in outs),
        in_specs=[vmem] * len(operands),
        out_specs=out_specs or tuple([vmem] * len(outs)),
        scratch_shapes=scratch,
    )(*operands)


def shifted(value, axis, by):
    n = lax.axis_size(axis)
    return lax.ppermute(value, axis, [(k, (k + by) % n) for k in range(n)])


def across(value, by_x, by_c):
    pairs = []
    for x in range(4):
        for c in range(2):
            pairs.append((2 * x + c, 2 * ((x + by_x) % 4) + (c ^ by_c)))
    return lax.ppermute(value, ("x", "c"), pairs)


def on_device(basis, residual, sigma, counts, pulsar, ecorr):
    groups = lax.axis_size("psr")
    slots, rows, width = basis.shape[2:]
    ndp = lax.axis_size(("z", "x", "c"))
    norm = float(ndp * slots * rows)
    every = norm * groups * groups
    keep, send = local_terms(basis[0], residual[0], sigma[0], counts[0], pulsar[0], ecorr)
    got = shifted(send, "c", 1)
    wire = ((2, 2 * HALF + 16, HALF), BF)
    outs = call(cores_kernel, "cores", [wire] * 3, [], (keep, got))
    arrived = [shifted(o, "psr", i + 1) for i, o in enumerate(outs)]
    own, *outs = call(
        unpack_kernel,
        "unpack",
        [((72, width), F32)] + [((80, width), BF)] * 7,
        [pltpu.VMEM((2, width, width), F32)],
        (keep, got, *arrived),
    )
    arrived = [across(o, (k + 1) // 2, (k + 1) % 2) for k, o in enumerate(outs)]
    kept, *outs = call(
        columns_kernel,
        "columns",
        [((24, width), F32)] + [((32, width), BF)] * 7,
        [pltpu.VMEM((2, 64, width), F32)],
        (own, *arrived),
    )
    arrived = [shifted(o, "z", k + 1) for k, o in enumerate(outs)]
    return call(
        functools.partial(final_kernel, norm, every),
        "final",
        [((PG, width // ndp, width), F32), ((PG, width // ndp), F32), ((2,), F32)],
        [],
        (kept, *arrived),
        (
            pl.BlockSpec(memory_space=pltpu.VMEM),
            pl.BlockSpec(memory_space=pltpu.VMEM),
            pl.BlockSpec(memory_space=pltpu.SMEM),
        ),
    )


def solution(mesh):
    finer = Mesh(mesh.devices.reshape(8, 4, 2, mesh.shape["psr"]), AXES)
    in_specs = (
        P(AXES, None, None, None, None),
        P(AXES, None, None, None),
        P(AXES, None, None, None),
        P(AXES, None, None),
        P(AXES, None, None),
        P(),
    )
    out_specs = (P("psr", ("z", "x", "c"), None), P("psr", ("z", "x", "c")), P())
    return jax.shard_map(
        on_device, mesh=finer, in_specs=in_specs, out_specs=out_specs, check_vma=False
    )
```

```python
import functools

import jax
import jax.numpy as jnp
from jax import lax
from jax.experimental import pallas as pl
from jax.experimental.pallas import tpu as pltpu
from jax.sharding import Mesh
from jax.sharding import PartitionSpec as P


PG = 4
AXES = ("z", "x", "c", "psr")
BF = jnp.bfloat16
F32 = jnp.float32
HALF = 128
GRANT = 16 * 2**20
DIRECT = (((0,), (0,)), ((), ()))


def split2(e):
    head = e.astype(BF).astype(F32)
    return jnp.concatenate([head, e - head], axis=0).astype(BF)


def joined2(x):
    full = x.astype(F32)
    rows = full.shape[0] // 2
    return full[:rows] + full[rows:]


def row_in(rows, width, items):
    sub = lax.broadcasted_iota(jnp.int32, (rows, width), 0)
    out = jnp.zeros((rows, width), F32)
    for at, item in items:
        out = jnp.where(sub == at, jnp.broadcast_to(item, (rows, width)), out)
    return out


def dot0(a, b):
    return lax.dot_general(a, b, DIRECT, preferred_element_type=F32)


def packed(full, rhs, totals):
    a = full[:HALF, :HALF]
    b = full[:HALF, HALF:]
    d = full[HALF:, HALF:]
    r = lax.broadcasted_iota(jnp.int32, (HALF, HALF), 0)
    c = lax.broadcasted_iota(jnp.int32, (HALF, HALF), 1)
    both = jnp.where(r >= c, a, d)
    diag = jnp.sum(jnp.where(r == c, d, 0.0), axis=0, keepdims=True)
    extras = row_in(
        8, HALF, [(0, diag), (1, rhs[:, :HALF]), (2, rhs[:, HALF:]), (3, totals)]
    )
    return b, both, extras


def terms_kernel(
    counts_h, pulsar_h, ecorr_h, sigma_h, residual_h, basis, keep, send,
    counts, pulsar, ecorr, sigma, residual, small_sems, buf, sems, acc, racc, inv_s, wide_s,
):
    groups, slots = counts.shape
    y = lax.axis_index("psr")
    core = lax.axis_index("c")
    small = [
        pltpu.make_async_copy(source, target, small_sems.at[k])
        for k, (source, target) in enumerate(
            (
                (counts_h, counts),
                (pulsar_h, pulsar),
                (ecorr_h, ecorr),
                (sigma_h, sigma),
                (residual_h, residual),
            )
        )
    ]
    for copy in small:
        copy.start()
    copies = []
    for i in range(groups):
        g = lax.rem(y + i, groups)
        copies.append(pltpu.make_async_copy(basis.at[g], buf.at[i], sems.at[i]))
        copies[-1].start()
    for copy in small:
        copy.wait()
    lane = lax.broadcasted_iota(jnp.int32, (slots, HALF), 1)
    sub = lax.broadcasted_iota(jnp.int32, (slots, HALF), 0)
    logdet = jnp.zeros((slots, 1), F32)
    chi = jnp.zeros((slots, 1), F32)
    for g in range(groups):
        count = jnp.zeros((slots, HALF), jnp.int32)
        amp = jnp.zeros((slots, HALF), F32)
        for s in range(slots):
            count = jnp.where(sub == s, counts[g, s], count)
            amp = jnp.where(sub == s, ecorr[g * PG + pulsar[g, s]], amp)
        sig = sigma[g].astype(F32)
        res = residual[g].astype(F32)
        square = sig * sig
        valid = lane < count
        inverse = jnp.where(valid, 1.0 / square, 0.0)
        scaled = inverse * res
        total = jnp.sum(inverse, axis=1, keepdims=True)
        wsum = jnp.sum(scaled, axis=1, keepdims=True)
        jitter = amp * amp
        grown = 1.0 + jitter * total
        coef = jitter / grown
        logs = jnp.sum(jnp.where(valid, jnp.log(square), 0.0), axis=1, keepdims=True)
        logdet = logdet + logs + jnp.log(grown)[:, :1]
        chi = chi + jnp.sum(scaled * res, axis=1, keepdims=True) - coef[:, :1] * wsum * wsum
        inv_s[g, 0] = inverse
        inv_s[g, 1] = res
        wide_s[g, 0] = coef
        wide_s[g, 1] = coef * wsum
    lane1 = lax.broadcasted_iota(jnp.int32, (1, HALF), 1)
    totals = jnp.where(
        lane1 == 0,
        jnp.sum(logdet, axis=0, keepdims=True),
        jnp.where(lane1 == 1, jnp.sum(chi, axis=0, keepdims=True), 0.0),
    )
    nothing = jnp.zeros((1, HALF), F32)
    for i in range(groups):
        g = lax.rem(y + i, groups)
        acc[...] = jnp.zeros_like(acc)
        racc[...] = jnp.zeros_like(racc)
        inverse_t = jnp.transpose(inv_s[g, 0])
        res_t = jnp.transpose(inv_s[g, 1])
        coef = wide_s[g, 0]
        pull = wide_s[g, 1]
        member = jnp.zeros((slots, HALF), jnp.int32)
        columns = []
        copies[i].wait()
        for s in range(slots):
            block = buf[i, s]
            weighted = (block.astype(F32) * inverse_t[:, s : s + 1]).astype(BF)
            weighted_f = weighted.astype(F32)
            column = jnp.sum(weighted_f, axis=0, keepdims=True)
            project = jnp.sum(weighted_f * res_t[:, s : s + 1], axis=0, keepdims=True)
            mine = pulsar[g, s]
            member = jnp.where(sub == s, mine, member)
            acc[mine] += dot0(block, weighted)
            racc[mine, 0:1, :] += project - pull[s : s + 1, 0:1] * column
            columns.append((s, column))
        cols = row_in(slots, 2 * HALF, columns)
        head = cols.astype(BF).astype(F32)
        rest = cols - head
        left = jnp.concatenate([head, rest, head, rest], axis=0).astype(BF)
        for at in range(PG):
            to = (core if at < 2 else 1 - core) * 2 + at % 2
            scale = jnp.where(member == to, coef, 0.0)
            scaled = jnp.concatenate([scale, scale], axis=1) * cols
            high = scaled.astype(BF).astype(F32)
            low = scaled - high
            right = jnp.concatenate([high, high, low, low], axis=0).astype(BF)
            full = acc[to] - dot0(left, right)
            b, both, extras = packed(
                full, racc[to, 0:1, :], totals if at % 2 == 0 else nothing
            )
            if at < 2:
                keep[i, at, 0:HALF, :] = b
                keep[i, at, HALF : 2 * HALF, :] = both
                keep[i, at, 2 * HALF :, :] = extras
            else:
                send[i, at - 2, 0:HALF, :] = b.astype(BF)
                send[i, at - 2, HALF : 2 * HALF, :] = both.astype(BF)
                send[i, at - 2, 2 * HALF :, :] = split2(extras)


def local_terms(basis, residual, sigma, counts, pulsar, ecorr):
    groups, slots, rows, width = basis.shape
    vmem = pl.BlockSpec(memory_space=pltpu.VMEM)
    return pl.pallas_call(
        terms_kernel,
        name="terms",
        out_shape=(
            jax.ShapeDtypeStruct((groups, 2, 2 * HALF + 8, HALF), F32),
            jax.ShapeDtypeStruct((groups, 2, 2 * HALF + 16, HALF), BF),
        ),
        in_specs=[pl.BlockSpec(memory_space=pltpu.HBM)] * 6,
        out_specs=(vmem, vmem),
        scratch_shapes=[
            pltpu.SMEM((groups, slots), jnp.int32),
            pltpu.SMEM((groups, slots), jnp.int32),
            pltpu.SMEM(ecorr.shape, F32),
            pltpu.VMEM((groups, slots, rows), BF),
            pltpu.VMEM((groups, slots, rows), BF),
            pltpu.SemaphoreType.DMA((5,)),
            pltpu.VMEM((groups, slots, rows, width), BF),
            pltpu.SemaphoreType.DMA((groups,)),
            pltpu.VMEM((PG, width, width), F32),
            pltpu.VMEM((PG, 8, width), F32),
            pltpu.VMEM((groups, 2, slots, rows), F32),
            pltpu.VMEM((groups, 2, slots, rows), F32),
        ],
    )(counts, pulsar, ecorr, sigma, residual, basis)


def cores_kernel(keep, got, *outs):
    for i, out in enumerate(outs):
        for j in range(2):
            body = keep[i + 1, j, : 2 * HALF] + got[i + 1, j, : 2 * HALF].astype(F32)
            out[j, : 2 * HALF] = body.astype(BF)
            out[j, 2 * HALF :] = split2(
                keep[i + 1, j, 2 * HALF :] + joined2(got[i + 1, j, 2 * HALF :])
            )


def own_spots():
    r = lax.broadcasted_iota(jnp.int32, (HALF, HALF), 0)
    c = lax.broadcasted_iota(jnp.int32, (HALF, HALF), 1)
    inside = (r // 4 == c // 4) & (r < c)
    r, c = r % 4, c % 4
    return (
        inside & (r == 0),
        inside & (r == 1) & (c == 2),
        inside & (r == 1) & (c == 3),
        inside & (r == 2),
    )


def with_extras(square, spots, before, after, head, rest):
    for spot, value in zip(spots, (before, after, head, rest)):
        square = jnp.where(spot, jnp.broadcast_to(value, square.shape), square)
    return square


def unpack_kernel(keep, got, *refs):
    arrived, out, full = refs[:-2], refs[-2], refs[-1]
    r = lax.broadcasted_iota(jnp.int32, (HALF, HALF), 0)
    c = lax.broadcasted_iota(jnp.int32, (HALF, HALF), 1)
    spots = own_spots()
    for j in range(2):
        body = keep[0, j, : 2 * HALF] + got[0, j, : 2 * HALF].astype(F32)
        extras = keep[0, j, 2 * HALF :] + joined2(got[0, j, 2 * HALF :])
        for a in arrived:
            body = body + a[j, : 2 * HALF].astype(F32)
            extras = extras + joined2(a[j, 2 * HALF :])
        b, both = body[:HALF], body[HALF:]
        flipped = jnp.transpose(both)
        if j == 0:
            totals = extras[3:4]
        value = totals[:, j : j + 1]
        head = value.astype(BF).astype(F32)
        before = jnp.roll(extras[1:3], 1, axis=1)
        after = jnp.roll(extras[1:3], HALF - 1, axis=1)
        low = jnp.where(r >= c, both, flipped)
        high = jnp.where(
            r < c, both, jnp.where(r > c, flipped, jnp.broadcast_to(extras[0:1], (HALF, HALF)))
        )
        full[j, :HALF, :HALF] = with_extras(
            low, spots, before[0:1], after[0:1], head, value - head
        )
        full[j, :HALF, HALF:] = b
        full[j, HALF:, :HALF] = jnp.transpose(b)
        full[j, HALF:, HALF:] = with_extras(
            high, spots, before[1:2], after[1:2], head, value - head
        )
    sub = lax.broadcasted_iota(jnp.int32, (8, 2 * HALF), 0)
    for m in range(out.shape[0] // 2):
        t0, t1 = full[0, 8 * m : 8 * m + 8], full[1, 8 * m : 8 * m + 8]
        out[2 * m] = jnp.where(sub < 4, t0, jnp.roll(t1, 4, axis=0)).astype(BF)
        out[2 * m + 1] = jnp.where(sub < 4, jnp.roll(t0, 4, axis=0), t1).astype(BF)


def final_kernel(norm, every, arrived, gram, rhs, totals):
    at = 8 * lax.axis_index("z") + 2 * lax.axis_index("x") + lax.axis_index("c")
    sides = []
    for core in range(2):
        side = arrived[core].astype(F32)
        for k in range(1, arrived.shape[0] // 2):
            side = side + arrived[2 * k + core].astype(F32)
        sides.append(side)
    block = jnp.concatenate(sides, axis=0)
    shape = block.shape
    lane = lax.broadcasted_iota(jnp.int32, shape, 1)
    sub = lax.rem(lax.broadcasted_iota(jnp.int32, shape, 0), 4)
    wide = [
        jnp.broadcast_to(
            jnp.sum(jnp.where(lane == 4 * at + k, block, 0.0), axis=1, keepdims=True), shape
        )
        for k in range(4)
    ]
    out = block
    for r in range(4):
        for c in range(r + 1, 4):
            mirror = jnp.roll(wide[r], r - c, axis=0)
            out = jnp.where((sub == r) & (lane == 4 * at + c), mirror, out)
    out = out * (1.0 / norm)
    spread = jnp.where(
        lane == 0,
        wide[1],
        jnp.where(lane == 1, wide[2], jnp.where(lane == 2, wide[3], jnp.roll(wide[2], -1, axis=0))),
    )
    spread = spread * (1.0 / norm)
    for q in range(PG):
        gram[q] = out[4 * q : 4 * q + 4]
        rhs[q : q + 1, :] = spread[4 * q : 4 * q + 1, 0:4]
    for k in range(2):
        totals[k] = (wide[3][4 * k + 1, 0] + wide[3][4 * k + 2, 0]) * (1.0 / every)


def call(kernel, name, outs, scratch, operands, out_specs=None):
    vmem = pl.BlockSpec(memory_space=pltpu.VMEM)
    return pl.pallas_call(
        kernel,
        name=name,
        out_shape=tuple(jax.ShapeDtypeStruct(s, d) for s, d in outs),
        in_specs=[vmem] * len(operands),
        out_specs=out_specs or tuple([vmem] * len(outs)),
        scratch_shapes=scratch,
        compiler_params=pltpu.CompilerParams(vmem_limit_bytes=GRANT),
    )(*operands)


def shifted(value, axis, by):
    n = lax.axis_size(axis)
    return lax.ppermute(value, axis, [(k, (k + by) % n) for k in range(n)])


def on_device(basis, residual, sigma, counts, pulsar, ecorr):
    groups = lax.axis_size("psr")
    slots, rows, width = basis.shape[2:]
    ndp = lax.axis_size(("z", "x", "c"))
    norm = float(ndp * slots * rows)
    every = norm * groups * groups
    keep, send = local_terms(basis[0], residual[0], sigma[0], counts[0], pulsar[0], ecorr)
    got = shifted(send, "c", 1)
    wire = ((2, 2 * HALF + 16, HALF), BF)
    outs = call(cores_kernel, "cores", [wire] * 3, [], (keep, got))
    arrived = [shifted(o, "psr", i + 1) for i, o in enumerate(outs)]
    (wire,) = call(
        unpack_kernel,
        "unpack",
        [((ndp, 8, width), BF)],
        [pltpu.VMEM((2, width, width), F32)],
        (keep, got, *arrived),
    )
    wire = lax.all_to_all(wire, ("z", "x", "c"), 0, 0, tiled=True)
    return call(
        functools.partial(final_kernel, norm, every),
        "final",
        [((PG, width // ndp, width), F32), ((PG, width // ndp), F32), ((2,), F32)],
        [],
        (wire,),
        (
            pl.BlockSpec(memory_space=pltpu.VMEM),
            pl.BlockSpec(memory_space=pltpu.VMEM),
            pl.BlockSpec(memory_space=pltpu.SMEM),
        ),
    )


def solution(mesh):
    finer = Mesh(mesh.devices.reshape(8, 4, 2, mesh.shape["psr"]), AXES)
    in_specs = (
        P(AXES, None, None, None, None),
        P(AXES, None, None, None),
        P(AXES, None, None, None),
        P(AXES, None, None),
        P(AXES, None, None),
        P(),
    )
    out_specs = (P("psr", ("z", "x", "c"), None), P("psr", ("z", "x", "c")), P())
    return jax.shard_map(
        on_device, mesh=finer, in_specs=in_specs, out_specs=out_specs, check_vma=False
    )
```

```python
import functools

import jax
import jax.numpy as jnp
from jax import lax
from jax.experimental import pallas as pl
from jax.experimental.pallas import tpu as pltpu
from jax.sharding import Mesh
from jax.sharding import PartitionSpec as P


PG = 4
AXES = ("z", "x", "c", "psr")
BF = jnp.bfloat16
F32 = jnp.float32
HALF = 128
GRANT = 16 * 2**20
DIRECT = (((0,), (0,)), ((), ()))


def split2(e):
    head = e.astype(BF).astype(F32)
    return jnp.concatenate([head, e - head], axis=0).astype(BF)


def joined2(x):
    full = x.astype(F32)
    rows = full.shape[0] // 2
    return full[:rows] + full[rows:]


def row_in(rows, width, items):
    sub = lax.broadcasted_iota(jnp.int32, (rows, width), 0)
    out = jnp.zeros((rows, width), F32)
    for at, item in items:
        out = jnp.where(sub == at, jnp.broadcast_to(item, (rows, width)), out)
    return out


def dot0(a, b):
    return lax.dot_general(a, b, DIRECT, preferred_element_type=F32)


def packed(full, rhs, totals):
    a = full[:HALF, :HALF]
    b = full[:HALF, HALF:]
    d = full[HALF:, HALF:]
    r = lax.broadcasted_iota(jnp.int32, (HALF, HALF), 0)
    c = lax.broadcasted_iota(jnp.int32, (HALF, HALF), 1)
    both = jnp.where(r >= c, a, d)
    diag = jnp.sum(jnp.where(r == c, d, 0.0), axis=0, keepdims=True)
    extras = row_in(
        8, HALF, [(0, diag), (1, rhs[:, :HALF]), (2, rhs[:, HALF:]), (3, totals)]
    )
    return b, both, extras


def terms_kernel(
    counts_h, pulsar_h, ecorr_h, sigma_h, residual_h, basis, keep, send,
    counts, pulsar, ecorr, sigma, residual, small_sems, buf, sems, acc, racc, inv_s, wide_s,
):
    groups, slots = counts.shape
    y = lax.axis_index("psr")
    core = lax.axis_index("c")
    small = [
        pltpu.make_async_copy(source, target, small_sems.at[k])
        for k, (source, target) in enumerate(
            (
                (counts_h, counts),
                (pulsar_h, pulsar),
                (ecorr_h, ecorr),
                (sigma_h, sigma),
                (residual_h, residual),
            )
        )
    ]
    for copy in small:
        copy.start()
    copies = []
    for i in range(groups):
        g = lax.rem(y + i, groups)
        copies.append(pltpu.make_async_copy(basis.at[g], buf.at[i], sems.at[i]))
        copies[-1].start()
    for copy in small:
        copy.wait()
    lane = lax.broadcasted_iota(jnp.int32, (slots, HALF), 1)
    sub = lax.broadcasted_iota(jnp.int32, (slots, HALF), 0)
    logdet = jnp.zeros((slots, 1), F32)
    chi = jnp.zeros((slots, 1), F32)
    for g in range(groups):
        count = jnp.zeros((slots, HALF), jnp.int32)
        amp = jnp.zeros((slots, HALF), F32)
        for s in range(slots):
            count = jnp.where(sub == s, counts[g, s], count)
            amp = jnp.where(sub == s, ecorr[g * PG + pulsar[g, s]], amp)
        sig = sigma[g].astype(F32)
        res = residual[g].astype(F32)
        square = sig * sig
        valid = lane < count
        inverse = jnp.where(valid, 1.0 / square, 0.0)
        scaled = inverse * res
        total = jnp.sum(inverse, axis=1, keepdims=True)
        wsum = jnp.sum(scaled, axis=1, keepdims=True)
        jitter = amp * amp
        grown = 1.0 + jitter * total
        coef = jitter / grown
        logs = jnp.sum(jnp.where(valid, jnp.log(square), 0.0), axis=1, keepdims=True)
        logdet = logdet + logs + jnp.log(grown)[:, :1]
        chi = chi + jnp.sum(scaled * res, axis=1, keepdims=True) - coef[:, :1] * wsum * wsum
        inv_s[g, 0] = inverse
        inv_s[g, 1] = res
        wide_s[g, 0] = coef
        wide_s[g, 1] = coef * wsum
    lane1 = lax.broadcasted_iota(jnp.int32, (1, HALF), 1)
    totals = jnp.where(
        lane1 == 0,
        jnp.sum(logdet, axis=0, keepdims=True),
        jnp.where(lane1 == 1, jnp.sum(chi, axis=0, keepdims=True), 0.0),
    )
    nothing = jnp.zeros((1, HALF), F32)
    for i in range(groups):
        g = lax.rem(y + i, groups)
        acc[...] = jnp.zeros_like(acc)
        racc[...] = jnp.zeros_like(racc)
        inverse_t = jnp.transpose(inv_s[g, 0])
        res_t = jnp.transpose(inv_s[g, 1])
        coef = wide_s[g, 0]
        pull = wide_s[g, 1]
        member = jnp.zeros((slots, HALF), jnp.int32)
        columns = []
        copies[i].wait()
        for s in range(slots):
            block = buf[i, s]
            weighted = (block.astype(F32) * inverse_t[:, s : s + 1]).astype(BF)
            weighted_f = weighted.astype(F32)
            column = jnp.sum(weighted_f, axis=0, keepdims=True)
            project = jnp.sum(weighted_f * res_t[:, s : s + 1], axis=0, keepdims=True)
            mine = pulsar[g, s]
            member = jnp.where(sub == s, mine, member)
            acc[mine] += dot0(block, weighted)
            racc[mine, 0:1, :] += project - pull[s : s + 1, 0:1] * column
            columns.append((s, column))
        cols = row_in(slots, 2 * HALF, columns)
        head = cols.astype(BF).astype(F32)
        rest = cols - head
        left = jnp.concatenate([head, rest, head, rest], axis=0).astype(BF)
        for at in range(PG):
            to = (core if at < 2 else 1 - core) * 2 + at % 2
            scale = jnp.where(member == to, coef, 0.0)
            scaled = jnp.concatenate([scale, scale], axis=1) * cols
            high = scaled.astype(BF).astype(F32)
            low = scaled - high
            right = jnp.concatenate([high, high, low, low], axis=0).astype(BF)
            full = acc[to] - dot0(left, right)
            b, both, extras = packed(
                full, racc[to, 0:1, :], totals if at % 2 == 0 else nothing
            )
            if at < 2:
                keep[i, at, 0:HALF, :] = b
                keep[i, at, HALF : 2 * HALF, :] = both
                keep[i, at, 2 * HALF :, :] = extras
            else:
                send[i, at - 2, 0:HALF, :] = b.astype(BF)
                send[i, at - 2, HALF : 2 * HALF, :] = both.astype(BF)
                send[i, at - 2, 2 * HALF :, :] = split2(extras)


def local_terms(basis, residual, sigma, counts, pulsar, ecorr):
    groups, slots, rows, width = basis.shape
    vmem = pl.BlockSpec(memory_space=pltpu.VMEM)
    return pl.pallas_call(
        terms_kernel,
        name="terms",
        out_shape=(
            jax.ShapeDtypeStruct((groups, 2, 2 * HALF + 8, HALF), F32),
            jax.ShapeDtypeStruct((groups, 2, 2 * HALF + 16, HALF), BF),
        ),
        in_specs=[pl.BlockSpec(memory_space=pltpu.HBM)] * 6,
        out_specs=(vmem, vmem),
        scratch_shapes=[
            pltpu.SMEM((groups, slots), jnp.int32),
            pltpu.SMEM((groups, slots), jnp.int32),
            pltpu.SMEM(ecorr.shape, F32),
            pltpu.VMEM((groups, slots, rows), BF),
            pltpu.VMEM((groups, slots, rows), BF),
            pltpu.SemaphoreType.DMA((5,)),
            pltpu.VMEM((groups, slots, rows, width), BF),
            pltpu.SemaphoreType.DMA((groups,)),
            pltpu.VMEM((PG, width, width), F32),
            pltpu.VMEM((PG, 8, width), F32),
            pltpu.VMEM((groups, 2, slots, rows), F32),
            pltpu.VMEM((groups, 2, slots, rows), F32),
        ],
        compiler_params=pltpu.CompilerParams(vmem_limit_bytes=GRANT),
    )(*[pltpu.with_memory_space_constraint(a, pltpu.HBM) for a in (counts, pulsar, ecorr, sigma, residual, basis)])


def cores_kernel(keep, got, *outs):
    for i, out in enumerate(outs):
        for j in range(2):
            body = keep[i + 1, j, : 2 * HALF] + got[i + 1, j, : 2 * HALF].astype(F32)
            out[j, : 2 * HALF] = body.astype(BF)
            out[j, 2 * HALF :] = split2(
                keep[i + 1, j, 2 * HALF :] + joined2(got[i + 1, j, 2 * HALF :])
            )


def own_spots():
    r = lax.broadcasted_iota(jnp.int32, (HALF, HALF), 0)
    c = lax.broadcasted_iota(jnp.int32, (HALF, HALF), 1)
    inside = (r // 4 == c // 4) & (r < c)
    r, c = r % 4, c % 4
    return (
        inside & (r == 0),
        inside & (r == 1) & (c == 2),
        inside & (r == 1) & (c == 3),
        inside & (r == 2),
    )


def with_extras(square, spots, before, after, head, rest):
    for spot, value in zip(spots, (before, after, head, rest)):
        square = jnp.where(spot, jnp.broadcast_to(value, square.shape), square)
    return square


def unpack_kernel(keep, got, *refs):
    arrived, out, full = refs[:-2], refs[-2], refs[-1]
    r = lax.broadcasted_iota(jnp.int32, (HALF, HALF), 0)
    c = lax.broadcasted_iota(jnp.int32, (HALF, HALF), 1)
    spots = own_spots()
    for j in range(2):
        body = keep[0, j, : 2 * HALF] + got[0, j, : 2 * HALF].astype(F32)
        extras = keep[0, j, 2 * HALF :] + joined2(got[0, j, 2 * HALF :])
        for a in arrived:
            body = body + a[j, : 2 * HALF].astype(F32)
            extras = extras + joined2(a[j, 2 * HALF :])
        b, both = body[:HALF], body[HALF:]
        flipped = jnp.transpose(both)
        if j == 0:
            totals = extras[3:4]
        value = totals[:, j : j + 1]
        head = value.astype(BF).astype(F32)
        before = jnp.roll(extras[1:3], 1, axis=1)
        after = jnp.roll(extras[1:3], HALF - 1, axis=1)
        low = jnp.where(r >= c, both, flipped)
        high = jnp.where(
            r < c, both, jnp.where(r > c, flipped, jnp.broadcast_to(extras[0:1], (HALF, HALF)))
        )
        full[j, :HALF, :HALF] = with_extras(
            low, spots, before[0:1], after[0:1], head, value - head
        )
        full[j, :HALF, HALF:] = b
        full[j, HALF:, :HALF] = jnp.transpose(b)
        full[j, HALF:, HALF:] = with_extras(
            high, spots, before[1:2], after[1:2], head, value - head
        )
    sub = lax.broadcasted_iota(jnp.int32, (8, 2 * HALF), 0)
    for m in range(out.shape[0] // 2):
        t0, t1 = full[0, 8 * m : 8 * m + 8], full[1, 8 * m : 8 * m + 8]
        out[2 * m] = jnp.where(sub < 4, t0, jnp.roll(t1, 4, axis=0)).astype(BF)
        out[2 * m + 1] = jnp.where(sub < 4, jnp.roll(t0, 4, axis=0), t1).astype(BF)


def final_kernel(norm, every, arrived, gram, rhs, totals):
    at = 8 * lax.axis_index("z") + 2 * lax.axis_index("x") + lax.axis_index("c")
    sides = []
    for core in range(2):
        side = arrived[core].astype(F32)
        for k in range(1, arrived.shape[0] // 2):
            side = side + arrived[2 * k + core].astype(F32)
        sides.append(side)
    block = jnp.concatenate(sides, axis=0)
    shape = block.shape
    lane = lax.broadcasted_iota(jnp.int32, shape, 1)
    sub = lax.rem(lax.broadcasted_iota(jnp.int32, shape, 0), 4)
    wide = [
        jnp.broadcast_to(
            jnp.sum(jnp.where(lane == 4 * at + k, block, 0.0), axis=1, keepdims=True), shape
        )
        for k in range(4)
    ]
    out = block
    for r in range(4):
        for c in range(r + 1, 4):
            mirror = jnp.roll(wide[r], r - c, axis=0)
            out = jnp.where((sub == r) & (lane == 4 * at + c), mirror, out)
    out = out * (1.0 / norm)
    spread = jnp.where(
        lane == 0,
        wide[1],
        jnp.where(lane == 1, wide[2], jnp.where(lane == 2, wide[3], jnp.roll(wide[2], -1, axis=0))),
    )
    spread = spread * (1.0 / norm)
    for q in range(PG):
        gram[q] = out[4 * q : 4 * q + 4]
        rhs[q : q + 1, :] = spread[4 * q : 4 * q + 1, 0:4]
    for k in range(2):
        totals[k] = (wide[3][4 * k + 1, 0] + wide[3][4 * k + 2, 0]) * (1.0 / every)


def call(kernel, name, outs, scratch, operands, out_specs=None):
    vmem = pl.BlockSpec(memory_space=pltpu.VMEM)
    return pl.pallas_call(
        kernel,
        name=name,
        out_shape=tuple(jax.ShapeDtypeStruct(s, d) for s, d in outs),
        in_specs=[vmem] * len(operands),
        out_specs=out_specs or tuple([vmem] * len(outs)),
        scratch_shapes=scratch,
        compiler_params=pltpu.CompilerParams(vmem_limit_bytes=GRANT),
    )(*operands)


def shifted(value, axis, by):
    n = lax.axis_size(axis)
    return lax.ppermute(value, axis, [(k, (k + by) % n) for k in range(n)])


def on_device(basis, residual, sigma, counts, pulsar, ecorr):
    groups = lax.axis_size("psr")
    slots, rows, width = basis.shape[2:]
    ndp = lax.axis_size(("z", "x", "c"))
    norm = float(ndp * slots * rows)
    every = norm * groups * groups
    keep, send = local_terms(basis[0], residual[0], sigma[0], counts[0], pulsar[0], ecorr)
    got = shifted(send, "c", 1)
    wire = ((2, 2 * HALF + 16, HALF), BF)
    outs = call(cores_kernel, "cores", [wire] * 3, [], (keep, got))
    arrived = [shifted(o, "psr", i + 1) for i, o in enumerate(outs)]
    (wire,) = call(
        unpack_kernel,
        "unpack",
        [((ndp, 8, width), BF)],
        [pltpu.VMEM((2, width, width), F32)],
        (keep, got, *arrived),
    )
    wire = lax.all_to_all(wire, ("z", "x", "c"), 0, 0, tiled=True)
    return call(
        functools.partial(final_kernel, norm, every),
        "final",
        [((PG, width // ndp, width), F32), ((PG, width // ndp), F32), ((2,), F32)],
        [],
        (wire,),
        (
            pl.BlockSpec(memory_space=pltpu.VMEM),
            pl.BlockSpec(memory_space=pltpu.VMEM),
            pl.BlockSpec(memory_space=pltpu.SMEM),
        ),
    )


def solution(mesh):
    finer = Mesh(mesh.devices.reshape(8, 4, 2, mesh.shape["psr"]), AXES)
    in_specs = (
        P(AXES, None, None, None, None),
        P(AXES, None, None, None),
        P(AXES, None, None, None),
        P(AXES, None, None),
        P(AXES, None, None),
        P(),
    )
    out_specs = (P("psr", ("z", "x", "c"), None), P("psr", ("z", "x", "c")), P())
    return jax.shard_map(
        on_device, mesh=finer, in_specs=in_specs, out_specs=out_specs, check_vma=False
    )
```

```python
import functools

import jax
import jax.numpy as jnp
from jax import lax
from jax.experimental import pallas as pl
from jax.experimental.pallas import tpu as pltpu
from jax.sharding import Mesh
from jax.sharding import PartitionSpec as P


PG = 4
ORDER = (2, 1, 3, 0)
AXES = ("z", "x", "c", "psr")
BF = jnp.bfloat16
F32 = jnp.float32
HALF = 128
GRANT = 16 * 2**20
DIRECT = (((0,), (0,)), ((), ()))


def split2(e):
    head = e.astype(BF).astype(F32)
    return jnp.concatenate([head, e - head], axis=0).astype(BF)


def joined2(x):
    full = x.astype(F32)
    rows = full.shape[0] // 2
    return full[:rows] + full[rows:]


def row_in(rows, width, items):
    sub = lax.broadcasted_iota(jnp.int32, (rows, width), 0)
    out = jnp.zeros((rows, width), F32)
    for at, item in items:
        out = jnp.where(sub == at, jnp.broadcast_to(item, (rows, width)), out)
    return out


def dot0(a, b):
    return lax.dot_general(a, b, DIRECT, preferred_element_type=F32)


def packed(full, rhs, totals):
    a = full[:HALF, :HALF]
    b = full[:HALF, HALF:]
    d = full[HALF:, HALF:]
    r = lax.broadcasted_iota(jnp.int32, (HALF, HALF), 0)
    c = lax.broadcasted_iota(jnp.int32, (HALF, HALF), 1)
    both = jnp.where(r >= c, a, d)
    diag = jnp.sum(jnp.where(r == c, d, 0.0), axis=0, keepdims=True)
    extras = row_in(
        8, HALF, [(0, diag), (1, rhs[:, :HALF]), (2, rhs[:, HALF:]), (3, totals)]
    )
    return b, both, extras


def prepare(i, g, counts, pulsar, ecorr, sigma, residual, rows_s, wide_s, member_s):
    slots = counts.shape[1]
    lane = lax.broadcasted_iota(jnp.int32, (slots, HALF), 1)
    sub = lax.broadcasted_iota(jnp.int32, (slots, HALF), 0)
    count = jnp.zeros((slots, HALF), jnp.int32)
    member = jnp.zeros((slots, HALF), jnp.int32)
    amp = jnp.zeros((slots, HALF), F32)
    for s in range(slots):
        mine = pulsar[g, s]
        count = jnp.where(sub == s, counts[g, s], count)
        member = jnp.where(sub == s, mine, member)
        amp = jnp.where(sub == s, ecorr[g * PG + mine], amp)
    sig = sigma[g].astype(F32)
    res = residual[g].astype(F32)
    square = sig * sig
    valid = lane < count
    inverse = jnp.where(valid, 1.0 / square, 0.0)
    scaled = inverse * res
    total = jnp.sum(inverse, axis=1, keepdims=True)
    wsum = jnp.sum(scaled, axis=1, keepdims=True)
    jitter = amp * amp
    grown = 1.0 + jitter * total
    coef = jitter / grown
    logs = jnp.sum(jnp.where(valid, jnp.log(square), 0.0), axis=1, keepdims=True)
    rows_s[i, 0] = inverse
    rows_s[i, 1] = res
    wide_s[i, 0] = coef
    wide_s[i, 1] = coef * wsum
    member_s[i] = member
    logdet = logs + jnp.log(grown)[:, :1]
    chi = jnp.sum(scaled * res, axis=1, keepdims=True) - coef[:, :1] * wsum * wsum
    return logdet, chi


def gram_of(at_out, blocks, rows, wide, member, totals, core, acc, racc, keep, send):
    slots = blocks.shape[0]
    acc[...] = jnp.zeros_like(acc)
    racc[...] = jnp.zeros_like(racc)
    inverse_t = jnp.transpose(rows[0])
    res_t = jnp.transpose(rows[1])
    coef, pull = wide[0], wide[1]
    columns = []
    for s in range(slots):
        block = blocks[s]
        weighted = (block.astype(F32) * inverse_t[:, s : s + 1]).astype(BF)
        weighted_f = weighted.astype(F32)
        column = jnp.sum(weighted_f, axis=0, keepdims=True)
        project = jnp.sum(weighted_f * res_t[:, s : s + 1], axis=0, keepdims=True)
        mine = member[s, 0]
        acc[mine] += dot0(block, weighted)
        racc[mine, 0:1, :] += project - pull[s : s + 1, 0:1] * column
        columns.append((s, column))
    cols = row_in(slots, 2 * HALF, columns)
    head = cols.astype(BF).astype(F32)
    rest = cols - head
    left = jnp.concatenate([head, rest, head, rest], axis=0).astype(BF)
    nothing = jnp.zeros((1, HALF), F32)
    for at in range(PG):
        to = (core if at < 2 else 1 - core) * 2 + at % 2
        scale = jnp.where(member == to, coef, 0.0)
        scaled = jnp.concatenate([scale, scale], axis=1) * cols
        high = scaled.astype(BF).astype(F32)
        low = scaled - high
        right = jnp.concatenate([high, high, low, low], axis=0).astype(BF)
        full = acc[to] - dot0(left, right)
        b, both, extras = packed(
            full, racc[to, 0:1, :], totals if at % 2 == 0 else nothing
        )
        if at < 2:
            keep[at_out, at, 0:HALF, :] = b
            keep[at_out, at, HALF : 2 * HALF, :] = both
            keep[at_out, at, 2 * HALF :, :] = extras
        else:
            send[at_out, at - 2, 0:HALF, :] = b.astype(BF)
            send[at_out, at - 2, HALF : 2 * HALF, :] = both.astype(BF)
            send[at_out, at - 2, 2 * HALF :, :] = split2(extras)


def first_kernel(
    counts_h, pulsar_h, ecorr_h, sigma_h, residual_h, basis,
    keep, send, later, rows_o, wide_o, member_o, totals_o,
    counts, pulsar, ecorr, sigma, residual, small_sems, buf, sems, acc, racc, rows_s, wide_s, member_s,
):
    y = lax.axis_index("psr")
    core = lax.axis_index("c")
    small = [
        pltpu.make_async_copy(source, target, small_sems.at[k])
        for k, (source, target) in enumerate(
            (
                (counts_h, counts),
                (pulsar_h, pulsar),
                (ecorr_h, ecorr),
                (sigma_h, sigma),
                (residual_h, residual),
            )
        )
    ]
    for copy in small:
        copy.start()
    copies = []
    for k, i in enumerate(ORDER):
        target = buf if k == 0 else later.at[k - 1]
        copies.append(pltpu.make_async_copy(basis.at[y ^ i], target, sems.at[k]))
        copies[-1].start()
    for copy in small:
        copy.wait()
    logdet, chi = 0.0, 0.0
    for k, i in enumerate(ORDER):
        places = (rows_s, wide_s, member_s, 0) if k == 0 else (rows_o, wide_o, member_o, k - 1)
        part = prepare(places[3], y ^ i, counts, pulsar, ecorr, sigma, residual, *places[:3])
        logdet, chi = logdet + part[0], chi + part[1]
    lane1 = lax.broadcasted_iota(jnp.int32, (1, HALF), 1)
    totals = jnp.where(
        lane1 == 0,
        jnp.sum(logdet, axis=0, keepdims=True),
        jnp.where(lane1 == 1, jnp.sum(chi, axis=0, keepdims=True), 0.0),
    )
    totals_o[...] = jnp.broadcast_to(totals, totals_o.shape)
    copies[0].wait()
    gram_of(0, buf, rows_s[0], wide_s[0], member_s[0], totals, core, acc, racc, keep, send)
    for copy in copies[1:]:
        copy.wait()


def later_kernel(which, later, rows, wide, member, totals, after, keep, send, acc, racc):
    core = lax.axis_index("c")
    for k, i in enumerate(which):
        gram_of(
            k, later.at[i], rows[i], wide[i], member[i], totals[0:1], core, acc, racc, keep, send
        )


def packs(n):
    return [((n, 2, 2 * HALF + 8, HALF), F32), ((n, 2, 2 * HALF + 16, HALF), BF)]


def accumulators(width):
    return [pltpu.VMEM((PG, width, width), F32), pltpu.VMEM((PG, 8, width), F32)]


def first_terms(basis, residual, sigma, counts, pulsar, ecorr):
    groups, slots, rows, width = basis.shape
    operands = (counts, pulsar, ecorr, sigma, residual, basis)
    return call(
        first_kernel,
        packs(1)
        + [
            ((groups - 1, slots, rows, width), BF),
            ((groups - 1, 2, slots, rows), F32),
            ((groups - 1, 2, slots, rows), F32),
            ((groups - 1, slots, rows), jnp.int32),
            ((8, HALF), F32),
        ],
        [
            pltpu.SMEM((groups, slots), jnp.int32),
            pltpu.SMEM((groups, slots), jnp.int32),
            pltpu.SMEM(ecorr.shape, F32),
            pltpu.VMEM((groups, slots, rows), BF),
            pltpu.VMEM((groups, slots, rows), BF),
            pltpu.SemaphoreType.DMA((5,)),
            pltpu.VMEM((slots, rows, width), BF),
            pltpu.SemaphoreType.DMA((groups,)),
            *accumulators(width),
            pltpu.VMEM((1, 2, slots, rows), F32),
            pltpu.VMEM((1, 2, slots, rows), F32),
            pltpu.VMEM((1, slots, rows), jnp.int32),
        ],
        [pltpu.with_memory_space_constraint(a, pltpu.HBM) for a in operands],
        in_specs=[pl.BlockSpec(memory_space=pltpu.HBM)] * 6,
    )


def later_terms(which, shared, after):
    vmem = pl.BlockSpec(memory_space=pltpu.VMEM)
    return call(
        functools.partial(later_kernel, which),
        packs(len(which)),
        accumulators(shared[0].shape[-1]),
        (*shared, after),
        in_specs=[vmem] * len(shared) + [pl.BlockSpec(memory_space=pl.ANY)],
        flops=len(which) * 10**9,
    )


def cores_kernel(at, keep, got, out):
    for j in range(2):
        body = keep[at, j, : 2 * HALF] + got[at, j, : 2 * HALF].astype(F32)
        out[j, : 2 * HALF] = body.astype(BF)
        out[j, 2 * HALF :] = split2(keep[at, j, 2 * HALF :] + joined2(got[at, j, 2 * HALF :]))


def own_spots():
    r = lax.broadcasted_iota(jnp.int32, (HALF, HALF), 0)
    c = lax.broadcasted_iota(jnp.int32, (HALF, HALF), 1)
    inside = (r // 4 == c // 4) & (r < c)
    r, c = r % 4, c % 4
    return (
        inside & (r == 0),
        inside & (r == 1) & (c == 2),
        inside & (r == 1) & (c == 3),
        inside & (r == 2),
    )


def with_extras(square, spots, before, after, head, rest):
    for spot, value in zip(spots, (before, after, head, rest)):
        square = jnp.where(spot, jnp.broadcast_to(value, square.shape), square)
    return square


def unpack_kernel(at, keep, got, *refs):
    arrived, out, full = refs[:-2], refs[-2], refs[-1]
    r = lax.broadcasted_iota(jnp.int32, (HALF, HALF), 0)
    c = lax.broadcasted_iota(jnp.int32, (HALF, HALF), 1)
    spots = own_spots()
    for j in range(2):
        body = keep[at, j, : 2 * HALF] + got[at, j, : 2 * HALF].astype(F32)
        extras = keep[at, j, 2 * HALF :] + joined2(got[at, j, 2 * HALF :])
        for a in arrived:
            body = body + a[j, : 2 * HALF].astype(F32)
            extras = extras + joined2(a[j, 2 * HALF :])
        b, both = body[:HALF], body[HALF:]
        flipped = jnp.transpose(both)
        if j == 0:
            totals = extras[3:4]
        value = totals[:, j : j + 1]
        head = value.astype(BF).astype(F32)
        before = jnp.roll(extras[1:3], 1, axis=1)
        after = jnp.roll(extras[1:3], HALF - 1, axis=1)
        low = jnp.where(r >= c, both, flipped)
        high = jnp.where(
            r < c, both, jnp.where(r > c, flipped, jnp.broadcast_to(extras[0:1], (HALF, HALF)))
        )
        full[j, :HALF, :HALF] = with_extras(
            low, spots, before[0:1], after[0:1], head, value - head
        )
        full[j, :HALF, HALF:] = b
        full[j, HALF:, :HALF] = jnp.transpose(b)
        full[j, HALF:, HALF:] = with_extras(
            high, spots, before[1:2], after[1:2], head, value - head
        )
    sub = lax.broadcasted_iota(jnp.int32, (8, 2 * HALF), 0)
    for m in range(out.shape[0] // 2):
        t0, t1 = full[0, 8 * m : 8 * m + 8], full[1, 8 * m : 8 * m + 8]
        out[2 * m] = jnp.where(sub < 4, t0, jnp.roll(t1, 4, axis=0)).astype(BF)
        out[2 * m + 1] = jnp.where(sub < 4, jnp.roll(t0, 4, axis=0), t1).astype(BF)


def final_kernel(norm, every, arrived, gram, rhs, totals):
    at = 8 * lax.axis_index("z") + 2 * lax.axis_index("x") + lax.axis_index("c")
    sides = []
    for core in range(2):
        side = arrived[core].astype(F32)
        for k in range(1, arrived.shape[0] // 2):
            side = side + arrived[2 * k + core].astype(F32)
        sides.append(side)
    block = jnp.concatenate(sides, axis=0)
    shape = block.shape
    lane = lax.broadcasted_iota(jnp.int32, shape, 1)
    sub = lax.rem(lax.broadcasted_iota(jnp.int32, shape, 0), 4)
    wide = [
        jnp.broadcast_to(
            jnp.sum(jnp.where(lane == 4 * at + k, block, 0.0), axis=1, keepdims=True), shape
        )
        for k in range(4)
    ]
    out = block
    for r in range(4):
        for c in range(r + 1, 4):
            mirror = jnp.roll(wide[r], r - c, axis=0)
            out = jnp.where((sub == r) & (lane == 4 * at + c), mirror, out)
    out = out * (1.0 / norm)
    spread = jnp.where(
        lane == 0,
        wide[1],
        jnp.where(lane == 1, wide[2], jnp.where(lane == 2, wide[3], jnp.roll(wide[2], -1, axis=0))),
    )
    spread = spread * (1.0 / norm)
    for q in range(PG):
        gram[q] = out[4 * q : 4 * q + 4]
        rhs[q : q + 1, :] = spread[4 * q : 4 * q + 1, 0:4]
    for k in range(2):
        totals[k] = (wide[3][4 * k + 1, 0] + wide[3][4 * k + 2, 0]) * (1.0 / every)


def call(kernel, outs, scratch, operands, out_specs=None, in_specs=None, flops=None):
    vmem = pl.BlockSpec(memory_space=pltpu.VMEM)
    cost = None
    if flops:
        cost = pl.CostEstimate(flops=flops, bytes_accessed=0, transcendentals=0)
    return pl.pallas_call(
        kernel,
        out_shape=tuple(jax.ShapeDtypeStruct(s, d) for s, d in outs),
        in_specs=in_specs or [vmem] * len(operands),
        out_specs=out_specs or tuple([vmem] * len(outs)),
        scratch_shapes=scratch,
        cost_estimate=cost,
        compiler_params=pltpu.CompilerParams(vmem_limit_bytes=GRANT),
    )(*operands)


def swapped(value, axis, by):
    return lax.ppermute(value, axis, [(k, k ^ by) for k in range(lax.axis_size(axis))])


def across_cores(at, keep, got):
    (out,) = call(
        functools.partial(cores_kernel, at), [((2, 2 * HALF + 16, HALF), BF)], [], (keep, got)
    )
    return out


def reduced(basis, residual, sigma, counts, pulsar, ecorr):
    groups = lax.axis_size("psr")
    slots, rows, width = basis.shape[2:]
    ndp = lax.axis_size(("z", "x", "c"))
    norm = float(ndp * slots * rows)
    every = norm * groups * groups
    keep, send, *shared = first_terms(
        basis[0], residual[0], sigma[0], counts[0], pulsar[0], ecorr
    )
    got = swapped(send, "c", 1)
    keep_b, send_b = later_terms((0,), shared, shared[-1])
    mine = across_cores(0, keep, got)
    arrived = [swapped(mine, "psr", ORDER[0])]
    got_b = swapped(send_b, "c", 1)
    keep, send = later_terms((1, 2), shared, mine)
    got = swapped(send, "c", 1)
    mine = across_cores(0, keep_b, got_b)
    arrived.append(swapped(mine, "psr", ORDER[1]))
    mine = across_cores(0, keep, got)
    arrived.append(swapped(mine, "psr", ORDER[2]))
    (wire,) = call(
        functools.partial(unpack_kernel, 1),
        [((ndp, 8, width), BF)],
        [pltpu.VMEM((2, width, width), F32)],
        (keep, got, *arrived),
    )
    wire = lax.all_to_all(wire, ("z", "x", "c"), 0, 0, tiled=True)
    return call(
        functools.partial(final_kernel, norm, every),
        [((PG, width // ndp, width), F32), ((PG, width // ndp), F32), ((2,), F32)],
        [],
        (wire,),
        (
            pl.BlockSpec(memory_space=pltpu.VMEM),
            pl.BlockSpec(memory_space=pltpu.VMEM),
            pl.BlockSpec(memory_space=pltpu.SMEM),
        ),
    )


def solution(mesh):
    finer = Mesh(mesh.devices.reshape(8, 4, 2, mesh.shape["psr"]), AXES)
    in_specs = (
        P(AXES, None, None, None, None),
        P(AXES, None, None, None),
        P(AXES, None, None, None),
        P(AXES, None, None),
        P(AXES, None, None),
        P(),
    )
    out_specs = (P("psr", ("z", "x", "c"), None), P("psr", ("z", "x", "c")), P())
    return jax.shard_map(
        reduced, mesh=finer, in_specs=in_specs, out_specs=out_specs, check_vma=False
    )
```

```python
import functools

import jax
import jax.numpy as jnp
from jax import lax
from jax.experimental import pallas as pl
from jax.experimental.pallas import tpu as pltpu
from jax.sharding import Mesh
from jax.sharding import PartitionSpec as P


PG = 4
ORDER = (2, 1, 3, 0)
AXES = ("z", "x", "c", "psr")
BF = jnp.bfloat16
F32 = jnp.float32
HALF = 128
GRANT = 16 * 2**20
DIRECT = (((0,), (0,)), ((), ()))


def split2(e):
    head = e.astype(BF).astype(F32)
    return jnp.concatenate([head, e - head], axis=0).astype(BF)


def joined2(x):
    full = x.astype(F32)
    rows = full.shape[0] // 2
    return full[:rows] + full[rows:]


def row_in(rows, width, items):
    sub = lax.broadcasted_iota(jnp.int32, (rows, width), 0)
    out = jnp.zeros((rows, width), F32)
    for at, item in items:
        out = jnp.where(sub == at, jnp.broadcast_to(item, (rows, width)), out)
    return out


def dot0(a, b):
    return lax.dot_general(a, b, DIRECT, preferred_element_type=F32)


def packed(full, rhs, totals):
    a = full[:HALF, :HALF]
    b = full[:HALF, HALF:]
    d = full[HALF:, HALF:]
    r = lax.broadcasted_iota(jnp.int32, (HALF, HALF), 0)
    c = lax.broadcasted_iota(jnp.int32, (HALF, HALF), 1)
    both = jnp.where(r >= c, a, d)
    diag = jnp.sum(jnp.where(r == c, d, 0.0), axis=0, keepdims=True)
    extras = row_in(
        8, HALF, [(0, diag), (1, rhs[:, :HALF]), (2, rhs[:, HALF:]), (3, totals)]
    )
    return b, both, extras


def prepare(i, g, counts, pulsar, ecorr, sigma, residual, rows_s, wide_s, member_s):
    slots = counts.shape[1]
    lane = lax.broadcasted_iota(jnp.int32, (slots, HALF), 1)
    sub = lax.broadcasted_iota(jnp.int32, (slots, HALF), 0)
    count = jnp.zeros((slots, HALF), jnp.int32)
    member = jnp.zeros((slots, HALF), jnp.int32)
    amp = jnp.zeros((slots, HALF), F32)
    for s in range(slots):
        mine = pulsar[g, s]
        count = jnp.where(sub == s, counts[g, s], count)
        member = jnp.where(sub == s, mine, member)
        amp = jnp.where(sub == s, ecorr[g * PG + mine], amp)
    sig = sigma[g].astype(F32)
    res = residual[g].astype(F32)
    square = sig * sig
    valid = lane < count
    inverse = jnp.where(valid, 1.0 / square, 0.0)
    scaled = inverse * res
    total = jnp.sum(inverse, axis=1, keepdims=True)
    wsum = jnp.sum(scaled, axis=1, keepdims=True)
    jitter = amp * amp
    grown = 1.0 + jitter * total
    coef = jitter / grown
    logs = jnp.sum(jnp.where(valid, jnp.log(square), 0.0), axis=1, keepdims=True)
    rows_s[i, 0] = inverse
    rows_s[i, 1] = res
    wide_s[i, 0] = coef
    wide_s[i, 1] = coef * wsum
    member_s[i] = member
    logdet = logs + jnp.log(grown)[:, :1]
    chi = jnp.sum(scaled * res, axis=1, keepdims=True) - coef[:, :1] * wsum * wsum
    return logdet, chi


def gram_of(at_out, blocks, rows, wide, member, totals, core, acc, racc, keep, send):
    slots = blocks.shape[0]
    acc[...] = jnp.zeros_like(acc)
    racc[...] = jnp.zeros_like(racc)
    inverse_t = jnp.transpose(rows[0])
    res_t = jnp.transpose(rows[1])
    coef, pull = wide[0], wide[1]
    columns = []
    for s in range(slots):
        block = blocks[s]
        weighted = (block.astype(F32) * inverse_t[:, s : s + 1]).astype(BF)
        weighted_f = weighted.astype(F32)
        column = jnp.sum(weighted_f, axis=0, keepdims=True)
        project = jnp.sum(weighted_f * res_t[:, s : s + 1], axis=0, keepdims=True)
        mine = member[s, 0]
        acc[mine] += dot0(block, weighted)
        racc[mine, 0:1, :] += project - pull[s : s + 1, 0:1] * column
        columns.append((s, column))
    cols = row_in(slots, 2 * HALF, columns)
    head = cols.astype(BF).astype(F32)
    rest = cols - head
    left = jnp.concatenate([head, rest, head, rest], axis=0).astype(BF)
    nothing = jnp.zeros((1, HALF), F32)
    for at in range(PG):
        to = (core if at < 2 else 1 - core) * 2 + at % 2
        scale = jnp.where(member == to, coef, 0.0)
        scaled = jnp.concatenate([scale, scale], axis=1) * cols
        high = scaled.astype(BF).astype(F32)
        low = scaled - high
        right = jnp.concatenate([high, high, low, low], axis=0).astype(BF)
        full = acc[to] - dot0(left, right)
        b, both, extras = packed(
            full, racc[to, 0:1, :], totals if at % 2 == 0 else nothing
        )
        if at < 2:
            keep[at_out, at, 0:HALF, :] = b
            keep[at_out, at, HALF : 2 * HALF, :] = both
            keep[at_out, at, 2 * HALF :, :] = extras
        else:
            send[at_out, at - 2, 0:HALF, :] = b.astype(BF)
            send[at_out, at - 2, HALF : 2 * HALF, :] = both.astype(BF)
            send[at_out, at - 2, 2 * HALF :, :] = split2(extras)


def first_kernel(
    counts_h, pulsar_h, ecorr_h, sigma_h, residual_h, basis,
    keep, send, later, rows_o, wide_o, member_o, totals_o,
    counts, pulsar, ecorr, sigma, residual, small_sems, buf, sems, acc, racc, rows_s, wide_s, member_s,
):
    groups = counts.shape[0]
    y = lax.axis_index("psr")
    core = lax.axis_index("c")
    small = [
        pltpu.make_async_copy(source, target, small_sems.at[k])
        for k, (source, target) in enumerate(
            (
                (counts_h, counts),
                (pulsar_h, pulsar),
                (ecorr_h, ecorr),
                (sigma_h, sigma),
                (residual_h, residual),
            )
        )
    ]
    for copy in small:
        copy.start()
    copies = []
    for k, i in enumerate(ORDER):
        target = buf if k == 0 else later.at[k - 1]
        copies.append(pltpu.make_async_copy(basis.at[lax.rem(y + i, groups)], target, sems.at[k]))
        copies[-1].start()
    for copy in small:
        copy.wait()
    logdet, chi = 0.0, 0.0
    for k, i in enumerate(ORDER):
        places = (rows_s, wide_s, member_s, 0) if k == 0 else (rows_o, wide_o, member_o, k - 1)
        g = lax.rem(y + i, groups)
        part = prepare(places[3], g, counts, pulsar, ecorr, sigma, residual, *places[:3])
        logdet, chi = logdet + part[0], chi + part[1]
    lane1 = lax.broadcasted_iota(jnp.int32, (1, HALF), 1)
    totals = jnp.where(
        lane1 == 0,
        jnp.sum(logdet, axis=0, keepdims=True),
        jnp.where(lane1 == 1, jnp.sum(chi, axis=0, keepdims=True), 0.0),
    )
    totals_o[...] = jnp.broadcast_to(totals, totals_o.shape)
    copies[0].wait()
    gram_of(0, buf, rows_s[0], wide_s[0], member_s[0], totals, core, acc, racc, keep, send)
    for copy in copies[1:]:
        copy.wait()


def later_kernel(which, later, rows, wide, member, totals, after, keep, send, acc, racc):
    core = lax.axis_index("c")
    for k, i in enumerate(which):
        gram_of(
            k, later.at[i], rows[i], wide[i], member[i], totals[0:1], core, acc, racc, keep, send
        )


def packs(n):
    return [((n, 2, 2 * HALF + 8, HALF), F32), ((n, 2, 2 * HALF + 16, HALF), BF)]


def accumulators(width):
    return [pltpu.VMEM((PG, width, width), F32), pltpu.VMEM((PG, 8, width), F32)]


def first_terms(basis, residual, sigma, counts, pulsar, ecorr):
    groups, slots, rows, width = basis.shape
    operands = (counts, pulsar, ecorr, sigma, residual, basis)
    return call(
        first_kernel,
        packs(1)
        + [
            ((groups - 1, slots, rows, width), BF),
            ((groups - 1, 2, slots, rows), F32),
            ((groups - 1, 2, slots, rows), F32),
            ((groups - 1, slots, rows), jnp.int32),
            ((8, HALF), F32),
        ],
        [
            pltpu.SMEM((groups, slots), jnp.int32),
            pltpu.SMEM((groups, slots), jnp.int32),
            pltpu.SMEM(ecorr.shape, F32),
            pltpu.VMEM((groups, slots, rows), BF),
            pltpu.VMEM((groups, slots, rows), BF),
            pltpu.SemaphoreType.DMA((5,)),
            pltpu.VMEM((slots, rows, width), BF),
            pltpu.SemaphoreType.DMA((groups,)),
            *accumulators(width),
            pltpu.VMEM((1, 2, slots, rows), F32),
            pltpu.VMEM((1, 2, slots, rows), F32),
            pltpu.VMEM((1, slots, rows), jnp.int32),
        ],
        [pltpu.with_memory_space_constraint(a, pltpu.HBM) for a in operands],
        in_specs=[pl.BlockSpec(memory_space=pltpu.HBM)] * 6,
    )


def later_terms(which, shared, after):
    vmem = pl.BlockSpec(memory_space=pltpu.VMEM)
    return call(
        functools.partial(later_kernel, which),
        packs(len(which)),
        accumulators(shared[0].shape[-1]),
        (*shared, after),
        in_specs=[vmem] * len(shared) + [pl.BlockSpec(memory_space=pl.ANY)],
        flops=len(which) * 10**9,
    )


def cores_kernel(at, relayed, keep, got, *refs):
    extra = refs[0] if relayed is not None else None
    for j in range(2):
        body = keep[at, j, : 2 * HALF] + got[at, j, : 2 * HALF].astype(F32)
        extras = keep[at, j, 2 * HALF :] + joined2(got[at, j, 2 * HALF :])
        if relayed == j:
            body = body + extra[: 2 * HALF].astype(F32)
            extras = extras + joined2(extra[2 * HALF :])
        out = refs[j] if relayed is None else refs[1].at[j]
        out[: 2 * HALF] = body.astype(BF)
        out[2 * HALF :] = split2(extras)


def own_spots():
    r = lax.broadcasted_iota(jnp.int32, (HALF, HALF), 0)
    c = lax.broadcasted_iota(jnp.int32, (HALF, HALF), 1)
    inside = (r // 4 == c // 4) & (r < c)
    r, c = r % 4, c % 4
    return (
        inside & (r == 0),
        inside & (r == 1) & (c == 2),
        inside & (r == 1) & (c == 3),
        inside & (r == 2),
    )


def with_extras(square, spots, before, after, head, rest):
    for spot, value in zip(spots, (before, after, head, rest)):
        square = jnp.where(spot, jnp.broadcast_to(value, square.shape), square)
    return square


def unpack_kernel(at, keep, got, *refs):
    arrived, out, full = refs[:-2], refs[-2], refs[-1]
    r = lax.broadcasted_iota(jnp.int32, (HALF, HALF), 0)
    c = lax.broadcasted_iota(jnp.int32, (HALF, HALF), 1)
    spots = own_spots()
    for j in range(2):
        body = keep[at, j, : 2 * HALF] + got[at, j, : 2 * HALF].astype(F32)
        extras = keep[at, j, 2 * HALF :] + joined2(got[at, j, 2 * HALF :])
        for a in arrived:
            body = body + a[j, : 2 * HALF].astype(F32)
            extras = extras + joined2(a[j, 2 * HALF :])
        b, both = body[:HALF], body[HALF:]
        flipped = jnp.transpose(both)
        if j == 0:
            totals = extras[3:4]
        value = totals[:, j : j + 1]
        head = value.astype(BF).astype(F32)
        before = jnp.roll(extras[1:3], 1, axis=1)
        after = jnp.roll(extras[1:3], HALF - 1, axis=1)
        low = jnp.where(r >= c, both, flipped)
        high = jnp.where(
            r < c, both, jnp.where(r > c, flipped, jnp.broadcast_to(extras[0:1], (HALF, HALF)))
        )
        full[j, :HALF, :HALF] = with_extras(
            low, spots, before[0:1], after[0:1], head, value - head
        )
        full[j, :HALF, HALF:] = b
        full[j, HALF:, :HALF] = jnp.transpose(b)
        full[j, HALF:, HALF:] = with_extras(
            high, spots, before[1:2], after[1:2], head, value - head
        )
    sub = lax.broadcasted_iota(jnp.int32, (8, 2 * HALF), 0)
    for m in range(out.shape[0] // 2):
        t0, t1 = full[0, 8 * m : 8 * m + 8], full[1, 8 * m : 8 * m + 8]
        out[2 * m] = jnp.where(sub < 4, t0, jnp.roll(t1, 4, axis=0)).astype(BF)
        out[2 * m + 1] = jnp.where(sub < 4, jnp.roll(t0, 4, axis=0), t1).astype(BF)


def final_kernel(norm, every, arrived, gram, rhs, totals):
    at = 8 * lax.axis_index("z") + 2 * lax.axis_index("x") + lax.axis_index("c")
    sides = []
    for core in range(2):
        side = arrived[core].astype(F32)
        for k in range(1, arrived.shape[0] // 2):
            side = side + arrived[2 * k + core].astype(F32)
        sides.append(side)
    block = jnp.concatenate(sides, axis=0)
    shape = block.shape
    lane = lax.broadcasted_iota(jnp.int32, shape, 1)
    sub = lax.rem(lax.broadcasted_iota(jnp.int32, shape, 0), 4)
    wide = [
        jnp.broadcast_to(
            jnp.sum(jnp.where(lane == 4 * at + k, block, 0.0), axis=1, keepdims=True), shape
        )
        for k in range(4)
    ]
    out = block
    for r in range(4):
        for c in range(r + 1, 4):
            mirror = jnp.roll(wide[r], r - c, axis=0)
            out = jnp.where((sub == r) & (lane == 4 * at + c), mirror, out)
    out = out * (1.0 / norm)
    spread = jnp.where(
        lane == 0,
        wide[1],
        jnp.where(lane == 1, wide[2], jnp.where(lane == 2, wide[3], jnp.roll(wide[2], -1, axis=0))),
    )
    spread = spread * (1.0 / norm)
    for q in range(PG):
        gram[q] = out[4 * q : 4 * q + 4]
        rhs[q : q + 1, :] = spread[4 * q : 4 * q + 1, 0:4]
    for k in range(2):
        totals[k] = (wide[3][4 * k + 1, 0] + wide[3][4 * k + 2, 0]) * (1.0 / every)


def call(kernel, outs, scratch, operands, out_specs=None, in_specs=None, flops=None):
    vmem = pl.BlockSpec(memory_space=pltpu.VMEM)
    cost = None
    if flops:
        cost = pl.CostEstimate(flops=flops, bytes_accessed=0, transcendentals=0)
    return pl.pallas_call(
        kernel,
        out_shape=tuple(jax.ShapeDtypeStruct(s, d) for s, d in outs),
        in_specs=in_specs or [vmem] * len(operands),
        out_specs=out_specs or tuple([vmem] * len(outs)),
        scratch_shapes=scratch,
        cost_estimate=cost,
        compiler_params=pltpu.CompilerParams(vmem_limit_bytes=GRANT),
    )(*operands)


def swapped(value, axis, by):
    return lax.ppermute(value, axis, [(k, k ^ by) for k in range(lax.axis_size(axis))])


def shifted(value, axis, by):
    n = lax.axis_size(axis)
    return lax.ppermute(value, axis, [(k, (k + by) % n) for k in range(n)])


def across_cores(at, keep, got, relayed=None, extra=None):
    wire = (2 * HALF + 16, HALF)
    outs = [(wire, BF)] * 2 if relayed is None else [((2, *wire), BF)]
    operands = (keep, got) if relayed is None else (keep, got, extra)
    return call(functools.partial(cores_kernel, at, relayed), outs, [], operands)


def reduced(basis, residual, sigma, counts, pulsar, ecorr):
    groups = lax.axis_size("psr")
    slots, rows, width = basis.shape[2:]
    ndp = lax.axis_size(("z", "x", "c"))
    norm = float(ndp * slots * rows)
    every = norm * groups * groups
    keep, send, *shared = first_terms(
        basis[0], residual[0], sigma[0], counts[0], pulsar[0], ecorr
    )
    got = swapped(send, "c", 1)
    keep_b, send_b = later_terms((0,), shared, shared[-1])
    up, down = across_cores(0, keep, got)
    from_below = shifted(up, "psr", 1)
    from_above = shifted(down, "psr", -1)
    got_b = swapped(send_b, "c", 1)
    keep, send = later_terms((1, 2), shared, up)
    got = swapped(send, "c", 1)
    (mine,) = across_cores(0, keep_b, got_b, 0, from_below)
    arrived = [shifted(mine, "psr", 1)]
    (mine,) = across_cores(0, keep, got, 1, from_above)
    arrived.append(shifted(mine, "psr", -1))
    (wire,) = call(
        functools.partial(unpack_kernel, 1),
        [((ndp, 8, width), BF)],
        [pltpu.VMEM((2, width, width), F32)],
        (keep, got, *arrived),
    )
    wire = lax.all_to_all(wire, ("z", "x", "c"), 0, 0, tiled=True)
    return call(
        functools.partial(final_kernel, norm, every),
        [((PG, width // ndp, width), F32), ((PG, width // ndp), F32), ((2,), F32)],
        [],
        (wire,),
        (
            pl.BlockSpec(memory_space=pltpu.VMEM),
            pl.BlockSpec(memory_space=pltpu.VMEM),
            pl.BlockSpec(memory_space=pltpu.SMEM),
        ),
    )


def solution(mesh):
    finer = Mesh(mesh.devices.reshape(8, 4, 2, mesh.shape["psr"]), AXES)
    in_specs = (
        P(AXES, None, None, None, None),
        P(AXES, None, None, None),
        P(AXES, None, None, None),
        P(AXES, None, None),
        P(AXES, None, None),
        P(),
    )
    out_specs = (P("psr", ("z", "x", "c"), None), P("psr", ("z", "x", "c")), P())
    return jax.shard_map(
        reduced, mesh=finer, in_specs=in_specs, out_specs=out_specs, check_vma=False
    )
```

```python
import functools

import jax
import jax.numpy as jnp
from jax import lax
from jax.experimental import pallas as pl
from jax.experimental.pallas import tpu as pltpu
from jax.sharding import Mesh
from jax.sharding import PartitionSpec as P


PG = 4
ORDER = (2, 1, 3, 0)
AXES = ("z", "x", "c", "psr")
BF = jnp.bfloat16
F32 = jnp.float32
HALF = 128
GRANT = 16 * 2**20
DIRECT = (((0,), (0,)), ((), ()))


def split2(e):
    head = e.astype(BF).astype(F32)
    return jnp.concatenate([head, e - head], axis=0).astype(BF)


def joined2(x):
    full = x.astype(F32)
    rows = full.shape[0] // 2
    return full[:rows] + full[rows:]


def row_in(rows, width, items):
    sub = lax.broadcasted_iota(jnp.int32, (rows, width), 0)
    out = jnp.zeros((rows, width), F32)
    for at, item in items:
        out = jnp.where(sub == at, jnp.broadcast_to(item, (rows, width)), out)
    return out


def dot0(a, b):
    return lax.dot_general(a, b, DIRECT, preferred_element_type=F32)


def packed(full, rhs, totals):
    a = full[:HALF, :HALF]
    b = full[:HALF, HALF:]
    d = full[HALF:, HALF:]
    r = lax.broadcasted_iota(jnp.int32, (HALF, HALF), 0)
    c = lax.broadcasted_iota(jnp.int32, (HALF, HALF), 1)
    both = jnp.where(r >= c, a, d)
    diag = jnp.sum(jnp.where(r == c, d, 0.0), axis=0, keepdims=True)
    extras = row_in(
        8, HALF, [(0, diag), (1, rhs[:, :HALF]), (2, rhs[:, HALF:]), (3, totals)]
    )
    return b, both, extras


def prepare(i, g, counts, pulsar, ecorr, sigma, residual, rows_s, wide_s, member_s):
    slots = counts.shape[1]
    lane = lax.broadcasted_iota(jnp.int32, (slots, HALF), 1)
    sub = lax.broadcasted_iota(jnp.int32, (slots, HALF), 0)
    count = jnp.zeros((slots, HALF), jnp.int32)
    member = jnp.zeros((slots, HALF), jnp.int32)
    amp = jnp.zeros((slots, HALF), F32)
    for s in range(slots):
        mine = pulsar[g, s]
        count = jnp.where(sub == s, counts[g, s], count)
        member = jnp.where(sub == s, mine, member)
        amp = jnp.where(sub == s, ecorr[g * PG + mine], amp)
    sig = sigma[g].astype(F32)
    res = residual[g].astype(F32)
    square = sig * sig
    valid = lane < count
    inverse = jnp.where(valid, 1.0 / square, 0.0)
    scaled = inverse * res
    total = jnp.sum(inverse, axis=1, keepdims=True)
    wsum = jnp.sum(scaled, axis=1, keepdims=True)
    jitter = amp * amp
    grown = 1.0 + jitter * total
    coef = jitter / grown
    logs = jnp.sum(jnp.where(valid, jnp.log(square), 0.0), axis=1, keepdims=True)
    rows_s[i, 0] = inverse
    rows_s[i, 1] = res
    wide_s[i, 0] = coef
    wide_s[i, 1] = coef * wsum
    member_s[i] = member
    logdet = logs + jnp.log(grown)[:, :1]
    chi = jnp.sum(scaled * res, axis=1, keepdims=True) - coef[:, :1] * wsum * wsum
    return logdet, chi


def gram_of(at_out, blocks, rows, wide, member, totals, core, acc, racc, keep, send):
    slots = blocks.shape[0]
    acc[...] = jnp.zeros_like(acc)
    racc[...] = jnp.zeros_like(racc)
    inverse_t = jnp.transpose(rows[0])
    res_t = jnp.transpose(rows[1])
    coef, pull = wide[0], wide[1]
    columns = []
    for s in range(slots):
        block = blocks[s]
        weighted = (block.astype(F32) * inverse_t[:, s : s + 1]).astype(BF)
        weighted_f = weighted.astype(F32)
        column = jnp.sum(weighted_f, axis=0, keepdims=True)
        project = jnp.sum(weighted_f * res_t[:, s : s + 1], axis=0, keepdims=True)
        mine = member[s, 0]
        acc[mine] += dot0(block, weighted)
        racc[mine, 0:1, :] += project - pull[s : s + 1, 0:1] * column
        columns.append((s, column))
    cols = row_in(slots, 2 * HALF, columns)
    head = cols.astype(BF).astype(F32)
    rest = cols - head
    left = jnp.concatenate([head, rest, head, rest], axis=0).astype(BF)
    nothing = jnp.zeros((1, HALF), F32)
    for at in range(PG):
        to = (core if at < 2 else 1 - core) * 2 + at % 2
        scale = jnp.where(member == to, coef, 0.0)
        scaled = jnp.concatenate([scale, scale], axis=1) * cols
        high = scaled.astype(BF).astype(F32)
        low = scaled - high
        right = jnp.concatenate([high, high, low, low], axis=0).astype(BF)
        full = acc[to] - dot0(left, right)
        b, both, extras = packed(
            full, racc[to, 0:1, :], totals if at % 2 == 0 else nothing
        )
        if at < 2:
            keep[at_out, at, 0:HALF, :] = b
            keep[at_out, at, HALF : 2 * HALF, :] = both
            keep[at_out, at, 2 * HALF :, :] = extras
        else:
            send[at_out, at - 2, 0:HALF, :] = b.astype(BF)
            send[at_out, at - 2, HALF : 2 * HALF, :] = both.astype(BF)
            send[at_out, at - 2, 2 * HALF :, :] = split2(extras)


def first_kernel(
    counts_h, pulsar_h, ecorr_h, sigma_h, residual_h, basis,
    keep, send, later, rows_o, wide_o, member_o, totals_o,
    counts, pulsar, ecorr, sigma, residual, small_sems, buf, sems, acc, racc, rows_s, wide_s, member_s,
):
    groups = counts.shape[0]
    y = lax.axis_index("psr")
    core = lax.axis_index("c")
    small = [
        pltpu.make_async_copy(source, target, small_sems.at[k])
        for k, (source, target) in enumerate(
            (
                (counts_h, counts),
                (pulsar_h, pulsar),
                (ecorr_h, ecorr),
                (sigma_h, sigma),
                (residual_h, residual),
            )
        )
    ]
    for copy in small:
        copy.start()
    copies = []
    for k, i in enumerate(ORDER):
        target = buf if k == 0 else later.at[k - 1]
        copies.append(pltpu.make_async_copy(basis.at[lax.rem(y + i, groups)], target, sems.at[k]))
        copies[-1].start()
    for copy in small:
        copy.wait()
    logdet, chi = 0.0, 0.0
    for k, i in enumerate(ORDER):
        places = (rows_s, wide_s, member_s, 0) if k == 0 else (rows_o, wide_o, member_o, k - 1)
        g = lax.rem(y + i, groups)
        part = prepare(places[3], g, counts, pulsar, ecorr, sigma, residual, *places[:3])
        logdet, chi = logdet + part[0], chi + part[1]
    lane1 = lax.broadcasted_iota(jnp.int32, (1, HALF), 1)
    totals = jnp.where(
        lane1 == 0,
        jnp.sum(logdet, axis=0, keepdims=True),
        jnp.where(lane1 == 1, jnp.sum(chi, axis=0, keepdims=True), 0.0),
    )
    totals_o[...] = jnp.broadcast_to(totals, totals_o.shape)
    copies[0].wait()
    gram_of(0, buf, rows_s[0], wide_s[0], member_s[0], totals, core, acc, racc, keep, send)
    for copy in copies[1:]:
        copy.wait()


def later_kernel(which, later, rows, wide, member, totals, after, keep, send, acc, racc):
    core = lax.axis_index("c")
    for k, i in enumerate(which):
        gram_of(
            k, later.at[i], rows[i], wide[i], member[i], totals[0:1], core, acc, racc, keep, send
        )


def packs(n):
    return [((n, 2, 2 * HALF + 8, HALF), F32), ((n, 2, 2 * HALF + 16, HALF), BF)]


def accumulators(width):
    return [pltpu.VMEM((PG, width, width), F32), pltpu.VMEM((PG, 8, width), F32)]


def first_terms(basis, residual, sigma, counts, pulsar, ecorr):
    groups, slots, rows, width = basis.shape
    operands = (counts, pulsar, ecorr, sigma, residual, basis)
    return call(
        first_kernel,
        packs(1)
        + [
            ((groups - 1, slots, rows, width), BF),
            ((groups - 1, 2, slots, rows), F32),
            ((groups - 1, 2, slots, rows), F32),
            ((groups - 1, slots, rows), jnp.int32),
            ((8, HALF), F32),
        ],
        [
            pltpu.SMEM((groups, slots), jnp.int32),
            pltpu.SMEM((groups, slots), jnp.int32),
            pltpu.SMEM(ecorr.shape, F32),
            pltpu.VMEM((groups, slots, rows), BF),
            pltpu.VMEM((groups, slots, rows), BF),
            pltpu.SemaphoreType.DMA((5,)),
            pltpu.VMEM((slots, rows, width), BF),
            pltpu.SemaphoreType.DMA((groups,)),
            *accumulators(width),
            pltpu.VMEM((1, 2, slots, rows), F32),
            pltpu.VMEM((1, 2, slots, rows), F32),
            pltpu.VMEM((1, slots, rows), jnp.int32),
        ],
        [pltpu.with_memory_space_constraint(a, pltpu.HBM) for a in operands],
        in_specs=[pl.BlockSpec(memory_space=pltpu.HBM)] * 6,
    )


def later_terms(which, shared, after):
    vmem = pl.BlockSpec(memory_space=pltpu.VMEM)
    return call(
        functools.partial(later_kernel, which),
        packs(len(which)),
        accumulators(shared[0].shape[-1]),
        (*shared, after),
        in_specs=[vmem] * len(shared) + [pl.BlockSpec(memory_space=pl.ANY)],
        flops=len(which) * 10**9,
    )


def cores_kernel(at, relayed, keep, got, *refs):
    extra = refs[0] if relayed is not None else None
    for j in range(2):
        body = keep[at, j, : 2 * HALF] + got[at, j, : 2 * HALF].astype(F32)
        extras = keep[at, j, 2 * HALF :] + joined2(got[at, j, 2 * HALF :])
        if relayed == j:
            body = body + extra[: 2 * HALF].astype(F32)
            extras = extras + joined2(extra[2 * HALF :])
        out = refs[j] if relayed is None else refs[1].at[j]
        out[: 2 * HALF] = body.astype(BF)
        out[2 * HALF :] = split2(extras)


def own_spots():
    r = lax.broadcasted_iota(jnp.int32, (HALF, HALF), 0)
    c = lax.broadcasted_iota(jnp.int32, (HALF, HALF), 1)
    inside = (r // 4 == c // 4) & (r < c)
    r, c = r % 4, c % 4
    return (
        inside & (r == 0),
        inside & (r == 1) & (c == 2),
        inside & (r == 1) & (c == 3),
        inside & (r == 2),
    )


def with_extras(square, spots, before, after, head, rest):
    for spot, value in zip(spots, (before, after, head, rest)):
        square = jnp.where(spot, jnp.broadcast_to(value, square.shape), square)
    return square


def unpack_kernel(at, keep, got, *refs):
    arrived, out, full = refs[:-2], refs[-2], refs[-1]
    r = lax.broadcasted_iota(jnp.int32, (HALF, HALF), 0)
    c = lax.broadcasted_iota(jnp.int32, (HALF, HALF), 1)
    spots = own_spots()
    for j in range(2):
        body = keep[at, j, : 2 * HALF] + got[at, j, : 2 * HALF].astype(F32)
        extras = keep[at, j, 2 * HALF :] + joined2(got[at, j, 2 * HALF :])
        for a in arrived:
            body = body + a[j, : 2 * HALF].astype(F32)
            extras = extras + joined2(a[j, 2 * HALF :])
        b, both = body[:HALF], body[HALF:]
        flipped = jnp.transpose(both)
        if j == 0:
            totals = extras[3:4]
        value = totals[:, j : j + 1]
        head = value.astype(BF).astype(F32)
        before = jnp.roll(extras[1:3], 1, axis=1)
        after = jnp.roll(extras[1:3], HALF - 1, axis=1)
        low = jnp.where(r >= c, both, flipped)
        high = jnp.where(
            r < c, both, jnp.where(r > c, flipped, jnp.broadcast_to(extras[0:1], (HALF, HALF)))
        )
        full[j, :HALF, :HALF] = with_extras(
            low, spots, before[0:1], after[0:1], head, value - head
        )
        full[j, :HALF, HALF:] = b
        full[j, HALF:, :HALF] = jnp.transpose(b)
        full[j, HALF:, HALF:] = with_extras(
            high, spots, before[1:2], after[1:2], head, value - head
        )
    sub = lax.broadcasted_iota(jnp.int32, (8, 2 * HALF), 0)
    n_x, n_z = lax.axis_size("x"), lax.axis_size("z")
    for m in range(n_z * n_x):
        to = 2 * ((m % n_x) * n_z + m // n_x)
        t0, t1 = full[0, 8 * m : 8 * m + 8], full[1, 8 * m : 8 * m + 8]
        out[to] = jnp.where(sub < 4, t0, jnp.roll(t1, 4, axis=0)).astype(BF)
        out[to + 1] = jnp.where(sub < 4, jnp.roll(t0, 4, axis=0), t1).astype(BF)


def final_kernel(norm, every, arrived, gram, rhs, totals):
    at = 8 * lax.axis_index("z") + 2 * lax.axis_index("x") + lax.axis_index("c")
    sides = []
    for core in range(2):
        side = arrived[core].astype(F32)
        for k in range(1, arrived.shape[0] // 2):
            side = side + arrived[2 * k + core].astype(F32)
        sides.append(side)
    block = jnp.concatenate(sides, axis=0)
    shape = block.shape
    lane = lax.broadcasted_iota(jnp.int32, shape, 1)
    sub = lax.rem(lax.broadcasted_iota(jnp.int32, shape, 0), 4)
    wide = [
        jnp.broadcast_to(
            jnp.sum(jnp.where(lane == 4 * at + k, block, 0.0), axis=1, keepdims=True), shape
        )
        for k in range(4)
    ]
    out = block
    for r in range(4):
        for c in range(r + 1, 4):
            mirror = jnp.roll(wide[r], r - c, axis=0)
            out = jnp.where((sub == r) & (lane == 4 * at + c), mirror, out)
    out = out * (1.0 / norm)
    spread = jnp.where(
        lane == 0,
        wide[1],
        jnp.where(lane == 1, wide[2], jnp.where(lane == 2, wide[3], jnp.roll(wide[2], -1, axis=0))),
    )
    spread = spread * (1.0 / norm)
    for q in range(PG):
        gram[q] = out[4 * q : 4 * q + 4]
        rhs[q : q + 1, :] = spread[4 * q : 4 * q + 1, 0:4]
    for k in range(2):
        totals[k] = (wide[3][4 * k + 1, 0] + wide[3][4 * k + 2, 0]) * (1.0 / every)


def call(kernel, outs, scratch, operands, out_specs=None, in_specs=None, flops=None):
    vmem = pl.BlockSpec(memory_space=pltpu.VMEM)
    cost = None
    if flops:
        cost = pl.CostEstimate(flops=flops, bytes_accessed=0, transcendentals=0)
    return pl.pallas_call(
        kernel,
        out_shape=tuple(jax.ShapeDtypeStruct(s, d) for s, d in outs),
        in_specs=in_specs or [vmem] * len(operands),
        out_specs=out_specs or tuple([vmem] * len(outs)),
        scratch_shapes=scratch,
        cost_estimate=cost,
        compiler_params=pltpu.CompilerParams(vmem_limit_bytes=GRANT),
    )(*operands)


def swapped(value, axis, by):
    return lax.ppermute(value, axis, [(k, k ^ by) for k in range(lax.axis_size(axis))])


def shifted(value, axis, by):
    n = lax.axis_size(axis)
    return lax.ppermute(value, axis, [(k, (k + by) % n) for k in range(n)])


def across_cores(at, keep, got, relayed=None, extra=None):
    wire = (2 * HALF + 16, HALF)
    outs = [(wire, BF)] * 2 if relayed is None else [((2, *wire), BF)]
    operands = (keep, got) if relayed is None else (keep, got, extra)
    return call(functools.partial(cores_kernel, at, relayed), outs, [], operands)


def reduced(basis, residual, sigma, counts, pulsar, ecorr):
    groups = lax.axis_size("psr")
    slots, rows, width = basis.shape[2:]
    ndp = lax.axis_size(("z", "x", "c"))
    norm = float(ndp * slots * rows)
    every = norm * groups * groups
    keep, send, *shared = first_terms(
        basis[0], residual[0], sigma[0], counts[0], pulsar[0], ecorr
    )
    got = swapped(send, "c", 1)
    keep_b, send_b = later_terms((0,), shared, shared[-1])
    up, down = across_cores(0, keep, got)
    from_below = shifted(up, "psr", 1)
    from_above = shifted(down, "psr", -1)
    got_b = swapped(send_b, "c", 1)
    keep, send = later_terms((1, 2), shared, up)
    got = swapped(send, "c", 1)
    (mine,) = across_cores(0, keep_b, got_b, 0, from_below)
    arrived = [shifted(mine, "psr", 1)]
    (mine,) = across_cores(0, keep, got, 1, from_above)
    arrived.append(shifted(mine, "psr", -1))
    (wire,) = call(
        functools.partial(unpack_kernel, 1),
        [((ndp, 8, width), BF)],
        [pltpu.VMEM((2, width, width), F32)],
        (keep, got, *arrived),
    )
    wire = lax.all_to_all(wire, ("x", "z", "c"), 0, 0, tiled=True)
    return call(
        functools.partial(final_kernel, norm, every),
        [((PG, width // ndp, width), F32), ((PG, width // ndp), F32), ((2,), F32)],
        [],
        (wire,),
        (
            pl.BlockSpec(memory_space=pltpu.VMEM),
            pl.BlockSpec(memory_space=pltpu.VMEM),
            pl.BlockSpec(memory_space=pltpu.SMEM),
        ),
    )


def solution(mesh):
    finer = Mesh(mesh.devices.reshape(8, 4, 2, mesh.shape["psr"]), AXES)
    in_specs = (
        P(AXES, None, None, None, None),
        P(AXES, None, None, None),
        P(AXES, None, None, None),
        P(AXES, None, None),
        P(AXES, None, None),
        P(),
    )
    out_specs = (P("psr", ("z", "x", "c"), None), P("psr", ("z", "x", "c")), P())
    return jax.shard_map(
        reduced, mesh=finer, in_specs=in_specs, out_specs=out_specs, check_vma=False
    )
```

```python
import functools

import jax
import jax.numpy as jnp
from jax import lax
from jax.experimental import pallas as pl
from jax.experimental.pallas import tpu as pltpu
from jax.sharding import Mesh
from jax.sharding import PartitionSpec as P


PG = 4
ORDER = (2, 1, 3, 0)
AXES = ("z", "x", "c", "psr")
BF = jnp.bfloat16
F32 = jnp.float32
HALF = 128
GRANT = 16 * 2**20
DIRECT = (((0,), (0,)), ((), ()))


def split2(e):
    head = e.astype(BF).astype(F32)
    return jnp.concatenate([head, e - head], axis=0).astype(BF)


def joined2(x):
    full = x.astype(F32)
    rows = full.shape[0] // 2
    return full[:rows] + full[rows:]


def row_in(rows, width, items):
    sub = lax.broadcasted_iota(jnp.int32, (rows, width), 0)
    out = jnp.zeros((rows, width), F32)
    for at, item in items:
        out = jnp.where(sub == at, jnp.broadcast_to(item, (rows, width)), out)
    return out


def dot0(a, b):
    return lax.dot_general(a, b, DIRECT, preferred_element_type=F32)


def packed(full, rhs, totals):
    a = full[:HALF, :HALF]
    b = full[:HALF, HALF:]
    d = full[HALF:, HALF:]
    r = lax.broadcasted_iota(jnp.int32, (HALF, HALF), 0)
    c = lax.broadcasted_iota(jnp.int32, (HALF, HALF), 1)
    both = jnp.where(r >= c, a, d)
    diag = jnp.sum(jnp.where(r == c, d, 0.0), axis=0, keepdims=True)
    extras = row_in(
        8, HALF, [(0, diag), (1, rhs[:, :HALF]), (2, rhs[:, HALF:]), (3, totals)]
    )
    return b, both, extras


def prepare(i, g, counts, pulsar, ecorr, sigma, residual, rows_s, wide_s, member_s):
    slots = counts.shape[1]
    lane = lax.broadcasted_iota(jnp.int32, (slots, HALF), 1)
    sub = lax.broadcasted_iota(jnp.int32, (slots, HALF), 0)
    count = jnp.zeros((slots, HALF), jnp.int32)
    member = jnp.zeros((slots, HALF), jnp.int32)
    amp = jnp.zeros((slots, HALF), F32)
    for s in range(slots):
        mine = pulsar[g, s]
        count = jnp.where(sub == s, counts[g, s], count)
        member = jnp.where(sub == s, mine, member)
        amp = jnp.where(sub == s, ecorr[g * PG + mine], amp)
    sig = sigma[g].astype(F32)
    res = residual[g].astype(F32)
    square = sig * sig
    valid = lane < count
    inverse = jnp.where(valid, 1.0 / square, 0.0)
    scaled = inverse * res
    total = jnp.sum(inverse, axis=1, keepdims=True)
    wsum = jnp.sum(scaled, axis=1, keepdims=True)
    jitter = amp * amp
    grown = 1.0 + jitter * total
    coef = jitter / grown
    logs = jnp.sum(jnp.where(valid, jnp.log(square), 0.0), axis=1, keepdims=True)
    rows_s[i, 0] = inverse
    rows_s[i, 1] = res
    wide_s[i, 0] = coef
    wide_s[i, 1] = coef * wsum
    member_s[i] = member
    logdet = logs + jnp.log(grown)[:, :1]
    chi = jnp.sum(scaled * res, axis=1, keepdims=True) - coef[:, :1] * wsum * wsum
    return logdet, chi


def gram_of(at_out, blocks, rows, wide, member, totals, core, acc, racc, keep, send):
    slots = blocks.shape[0]
    acc[...] = jnp.zeros_like(acc)
    racc[...] = jnp.zeros_like(racc)
    inverse_t = jnp.transpose(rows[0])
    res_t = jnp.transpose(rows[1])
    coef, pull = wide[0], wide[1]
    columns = []
    for s in range(slots):
        block = blocks[s]
        weighted = (block.astype(F32) * inverse_t[:, s : s + 1]).astype(BF)
        weighted_f = weighted.astype(F32)
        column = jnp.sum(weighted_f, axis=0, keepdims=True)
        project = jnp.sum(weighted_f * res_t[:, s : s + 1], axis=0, keepdims=True)
        mine = member[s, 0]
        acc[mine] += dot0(block, weighted)
        racc[mine, 0:1, :] += project - pull[s : s + 1, 0:1] * column
        columns.append((s, column))
    cols = row_in(slots, 2 * HALF, columns)
    head = cols.astype(BF).astype(F32)
    rest = cols - head
    left = jnp.concatenate([head, rest, head, rest], axis=0).astype(BF)
    nothing = jnp.zeros((1, HALF), F32)
    for at in range(PG):
        to = (core if at < 2 else 1 - core) * 2 + at % 2
        scale = jnp.where(member == to, coef, 0.0)
        scaled = jnp.concatenate([scale, scale], axis=1) * cols
        high = scaled.astype(BF).astype(F32)
        low = scaled - high
        right = jnp.concatenate([high, high, low, low], axis=0).astype(BF)
        full = acc[to] - dot0(left, right)
        b, both, extras = packed(
            full, racc[to, 0:1, :], totals if at % 2 == 0 else nothing
        )
        if at < 2:
            keep[at_out, at, 0:HALF, :] = b
            keep[at_out, at, HALF : 2 * HALF, :] = both
            keep[at_out, at, 2 * HALF :, :] = extras
        else:
            send[at_out, at - 2, 0:HALF, :] = b.astype(BF)
            send[at_out, at - 2, HALF : 2 * HALF, :] = both.astype(BF)
            send[at_out, at - 2, 2 * HALF :, :] = split2(extras)


def first_kernel(
    counts_h, pulsar_h, ecorr_h, sigma_h, residual_h, basis,
    keep, send, later, rows_o, wide_o, member_o, totals_o,
    counts, pulsar, ecorr, sigma, residual, small_sems, buf, sems, acc, racc, rows_s, wide_s, member_s,
):
    groups = counts.shape[0]
    y = lax.axis_index("psr")
    core = lax.axis_index("c")
    small = [
        pltpu.make_async_copy(source, target, small_sems.at[k])
        for k, (source, target) in enumerate(
            (
                (counts_h, counts),
                (pulsar_h, pulsar),
                (ecorr_h, ecorr),
                (sigma_h, sigma),
                (residual_h, residual),
            )
        )
    ]
    for copy in small:
        copy.start()
    copies = []
    for k, i in enumerate(ORDER):
        target = buf if k == 0 else later.at[k - 1]
        copies.append(pltpu.make_async_copy(basis.at[lax.rem(y + i, groups)], target, sems.at[k]))
        copies[-1].start()
    for copy in small:
        copy.wait()
    logdet, chi = 0.0, 0.0
    for k, i in enumerate(ORDER):
        places = (rows_s, wide_s, member_s, 0) if k == 0 else (rows_o, wide_o, member_o, k - 1)
        g = lax.rem(y + i, groups)
        part = prepare(places[3], g, counts, pulsar, ecorr, sigma, residual, *places[:3])
        logdet, chi = logdet + part[0], chi + part[1]
    lane1 = lax.broadcasted_iota(jnp.int32, (1, HALF), 1)
    totals = jnp.where(
        lane1 == 0,
        jnp.sum(logdet, axis=0, keepdims=True),
        jnp.where(lane1 == 1, jnp.sum(chi, axis=0, keepdims=True), 0.0),
    )
    totals_o[...] = jnp.broadcast_to(totals, totals_o.shape)
    copies[0].wait()
    gram_of(0, buf, rows_s[0], wide_s[0], member_s[0], totals, core, acc, racc, keep, send)
    for copy in copies[1:]:
        copy.wait()


def later_kernel(which, later, rows, wide, member, totals, after, keep, send, acc, racc):
    core = lax.axis_index("c")
    for k, i in enumerate(which):
        gram_of(
            k, later.at[i], rows[i], wide[i], member[i], totals[0:1], core, acc, racc, keep, send
        )


def packs(n):
    return [((n, 2, 2 * HALF + 8, HALF), F32), ((n, 2, 2 * HALF + 16, HALF), BF)]


def accumulators(width):
    return [pltpu.VMEM((PG, width, width), F32), pltpu.VMEM((PG, 8, width), F32)]


def first_terms(basis, residual, sigma, counts, pulsar, ecorr):
    groups, slots, rows, width = basis.shape
    operands = (counts, pulsar, ecorr, sigma, residual, basis)
    return call(
        first_kernel,
        packs(1)
        + [
            ((groups - 1, slots, rows, width), BF),
            ((groups - 1, 2, slots, rows), F32),
            ((groups - 1, 2, slots, rows), F32),
            ((groups - 1, slots, rows), jnp.int32),
            ((8, HALF), F32),
        ],
        [
            pltpu.SMEM((groups, slots), jnp.int32),
            pltpu.SMEM((groups, slots), jnp.int32),
            pltpu.SMEM(ecorr.shape, F32),
            pltpu.VMEM((groups, slots, rows), BF),
            pltpu.VMEM((groups, slots, rows), BF),
            pltpu.SemaphoreType.DMA((5,)),
            pltpu.VMEM((slots, rows, width), BF),
            pltpu.SemaphoreType.DMA((groups,)),
            *accumulators(width),
            pltpu.VMEM((1, 2, slots, rows), F32),
            pltpu.VMEM((1, 2, slots, rows), F32),
            pltpu.VMEM((1, slots, rows), jnp.int32),
        ],
        [pltpu.with_memory_space_constraint(a, pltpu.HBM) for a in operands],
        in_specs=[pl.BlockSpec(memory_space=pltpu.HBM)] * 6,
    )


def later_terms(which, shared, after):
    vmem = pl.BlockSpec(memory_space=pltpu.VMEM)
    return call(
        functools.partial(later_kernel, which),
        packs(len(which)),
        accumulators(shared[0].shape[-1]),
        (*shared, after),
        in_specs=[vmem] * len(shared) + [pl.BlockSpec(memory_space=pl.ANY)],
        flops=len(which) * 10**9,
    )


def cores_kernel(at, relayed, keep, got, *refs):
    extra = refs[0] if relayed is not None else None
    for j in range(2):
        body = keep[at, j, : 2 * HALF] + got[at, j, : 2 * HALF].astype(F32)
        extras = keep[at, j, 2 * HALF :] + joined2(got[at, j, 2 * HALF :])
        if relayed == j:
            body = body + extra[: 2 * HALF].astype(F32)
            extras = extras + joined2(extra[2 * HALF :])
        out = refs[j] if relayed is None else refs[1].at[j]
        out[: 2 * HALF] = body.astype(BF)
        out[2 * HALF :] = split2(extras)


def own_spots():
    r = lax.broadcasted_iota(jnp.int32, (HALF, HALF), 0)
    c = lax.broadcasted_iota(jnp.int32, (HALF, HALF), 1)
    inside = (r // 4 == c // 4) & (r < c)
    r, c = r % 4, c % 4
    return (
        inside & (r == 0),
        inside & (r == 1) & (c == 2),
        inside & (r == 1) & (c == 3),
        inside & (r == 2),
    )


def with_extras(square, spots, before, after, head, rest):
    for spot, value in zip(spots, (before, after, head, rest)):
        square = jnp.where(spot, jnp.broadcast_to(value, square.shape), square)
    return square


def unpack_kernel(at, keep, got, *refs):
    arrived, out, full = refs[:-2], refs[-2], refs[-1]
    r = lax.broadcasted_iota(jnp.int32, (HALF, HALF), 0)
    c = lax.broadcasted_iota(jnp.int32, (HALF, HALF), 1)
    spots = own_spots()
    for j in range(2):
        body = keep[at, j, : 2 * HALF] + got[at, j, : 2 * HALF].astype(F32)
        extras = keep[at, j, 2 * HALF :] + joined2(got[at, j, 2 * HALF :])
        for a in arrived:
            body = body + a[j, : 2 * HALF].astype(F32)
            extras = extras + joined2(a[j, 2 * HALF :])
        b, both = body[:HALF], body[HALF:]
        flipped = jnp.transpose(both)
        if j == 0:
            totals = extras[3:4]
        value = totals[:, j : j + 1]
        head = value.astype(BF).astype(F32)
        before = jnp.roll(extras[1:3], 1, axis=1)
        after = jnp.roll(extras[1:3], HALF - 1, axis=1)
        low = jnp.where(r >= c, both, flipped)
        high = jnp.where(
            r < c, both, jnp.where(r > c, flipped, jnp.broadcast_to(extras[0:1], (HALF, HALF)))
        )
        full[j, :HALF, :HALF] = with_extras(
            low, spots, before[0:1], after[0:1], head, value - head
        )
        full[j, :HALF, HALF:] = b
        full[j, HALF:, :HALF] = jnp.transpose(b)
        full[j, HALF:, HALF:] = with_extras(
            high, spots, before[1:2], after[1:2], head, value - head
        )
    sub = lax.broadcasted_iota(jnp.int32, (8, 2 * HALF), 0)
    n_x, n_z = lax.axis_size("x"), lax.axis_size("z")
    for m in range(n_z * n_x):
        to = 2 * ((m % n_x) * n_z + m // n_x)
        t0, t1 = full[0, 8 * m : 8 * m + 8], full[1, 8 * m : 8 * m + 8]
        out[to] = jnp.where(sub < 4, t0, jnp.roll(t1, 4, axis=0)).astype(BF)
        out[to + 1] = jnp.where(sub < 4, jnp.roll(t0, 4, axis=0), t1).astype(BF)


def final_kernel(norm, every, arrived, gram, rhs, totals):
    at = 8 * lax.axis_index("z") + 2 * lax.axis_index("x") + lax.axis_index("c")
    sides = []
    for core in range(2):
        side = arrived[core].astype(F32)
        for k in range(1, arrived.shape[0] // 2):
            side = side + arrived[2 * k + core].astype(F32)
        sides.append(side)
    block = jnp.concatenate(sides, axis=0)
    shape = block.shape
    lane = lax.broadcasted_iota(jnp.int32, shape, 1)
    sub = lax.rem(lax.broadcasted_iota(jnp.int32, shape, 0), 4)
    wide = [
        jnp.broadcast_to(
            jnp.sum(jnp.where(lane == 4 * at + k, block, 0.0), axis=1, keepdims=True), shape
        )
        for k in range(4)
    ]
    out = block
    for r in range(4):
        for c in range(r + 1, 4):
            mirror = jnp.roll(wide[r], r - c, axis=0)
            out = jnp.where((sub == r) & (lane == 4 * at + c), mirror, out)
    out = out * (1.0 / norm)
    spread = jnp.where(
        lane == 0,
        wide[1],
        jnp.where(lane == 1, wide[2], jnp.where(lane == 2, wide[3], jnp.roll(wide[2], -1, axis=0))),
    )
    spread = spread * (1.0 / norm)
    for q in range(PG):
        gram[q] = out[4 * q : 4 * q + 4]
        rhs[q : q + 1, :] = spread[4 * q : 4 * q + 1, 0:4]
    for k in range(2):
        totals[k] = (wide[3][4 * k + 1, 0] + wide[3][4 * k + 2, 0]) * (1.0 / every)


def call(kernel, outs, scratch, operands, out_specs=None, in_specs=None, flops=None):
    vmem = pl.BlockSpec(memory_space=pltpu.VMEM)
    cost = None
    if flops:
        cost = pl.CostEstimate(flops=flops, bytes_accessed=0, transcendentals=0)
    return pl.pallas_call(
        kernel,
        out_shape=tuple(jax.ShapeDtypeStruct(s, d) for s, d in outs),
        in_specs=in_specs or [vmem] * len(operands),
        out_specs=out_specs or tuple([vmem] * len(outs)),
        scratch_shapes=scratch,
        cost_estimate=cost,
        compiler_params=pltpu.CompilerParams(vmem_limit_bytes=GRANT),
    )(*operands)


def swapped(value, axis, by):
    return lax.ppermute(value, axis, [(k, k ^ by) for k in range(lax.axis_size(axis))])


def shifted(value, axis, by):
    n = lax.axis_size(axis)
    return lax.ppermute(value, axis, [(k, (k + by) % n) for k in range(n)])


def across_cores(at, keep, got, relayed=None, extra=None):
    wire = (2 * HALF + 16, HALF)
    outs = [(wire, BF)] * 2 if relayed is None else [((2, *wire), BF)]
    operands = (keep, got) if relayed is None else (keep, got, extra)
    return call(functools.partial(cores_kernel, at, relayed), outs, [], operands)


def reduced(basis, residual, sigma, counts, pulsar, ecorr):
    groups = lax.axis_size("psr")
    slots, rows, width = basis.shape[2:]
    ndp = lax.axis_size(("z", "x", "c"))
    norm = float(ndp * slots * rows)
    every = norm * groups * groups
    keep, send, *shared = first_terms(
        basis[0], residual[0], sigma[0], counts[0], pulsar[0], ecorr
    )
    got = swapped(send, "c", 1)
    keep_b, send_b = later_terms((0,), shared, shared[-1])
    up, down = across_cores(0, keep, got)
    from_below = shifted(up, "psr", 1)
    from_above = shifted(down, "psr", -1)
    got_b = swapped(send_b, "c", 1)
    keep_c, send_c = later_terms((1,), shared, up)
    got_c = swapped(send_c, "c", 1)
    keep, send = later_terms((2,), shared, keep_c)
    got = swapped(send, "c", 1)
    (mine,) = across_cores(0, keep_b, got_b, 0, from_below)
    arrived = [shifted(mine, "psr", 1)]
    (mine,) = across_cores(0, keep_c, got_c, 1, from_above)
    arrived.append(shifted(mine, "psr", -1))
    (wire,) = call(
        functools.partial(unpack_kernel, 0),
        [((ndp, 8, width), BF)],
        [pltpu.VMEM((2, width, width), F32)],
        (keep, got, *arrived),
    )
    wire = lax.all_to_all(wire, ("x", "z", "c"), 0, 0, tiled=True)
    return call(
        functools.partial(final_kernel, norm, every),
        [((PG, width // ndp, width), F32), ((PG, width // ndp), F32), ((2,), F32)],
        [],
        (wire,),
        (
            pl.BlockSpec(memory_space=pltpu.VMEM),
            pl.BlockSpec(memory_space=pltpu.VMEM),
            pl.BlockSpec(memory_space=pltpu.SMEM),
        ),
    )


def solution(mesh):
    finer = Mesh(mesh.devices.reshape(8, 4, 2, mesh.shape["psr"]), AXES)
    in_specs = (
        P(AXES, None, None, None, None),
        P(AXES, None, None, None),
        P(AXES, None, None, None),
        P(AXES, None, None),
        P(AXES, None, None),
        P(),
    )
    out_specs = (P("psr", ("z", "x", "c"), None), P("psr", ("z", "x", "c")), P())
    return jax.shard_map(
        reduced, mesh=finer, in_specs=in_specs, out_specs=out_specs, check_vma=False
    )
```

```python
import functools

import jax
import jax.numpy as jnp
from jax import lax
from jax.experimental import pallas as pl
from jax.experimental.pallas import tpu as pltpu
from jax.sharding import Mesh
from jax.sharding import PartitionSpec as P


PG = 4
ORDER = (2, 1, 3, 0)
AXES = ("z", "x", "c", "psr")
BF = jnp.bfloat16
F32 = jnp.float32
HALF = 128
GRANT = 16 * 2**20
DIRECT = (((0,), (0,)), ((), ()))


def split2(e):
    head = e.astype(BF).astype(F32)
    return jnp.concatenate([head, e - head], axis=0).astype(BF)


def joined2(x):
    full = x.astype(F32)
    rows = full.shape[0] // 2
    return full[:rows] + full[rows:]


def row_in(rows, width, items):
    sub = lax.broadcasted_iota(jnp.int32, (rows, width), 0)
    out = jnp.zeros((rows, width), F32)
    for at, item in items:
        out = jnp.where(sub == at, jnp.broadcast_to(item, (rows, width)), out)
    return out


def dot0(a, b):
    return lax.dot_general(a, b, DIRECT, preferred_element_type=F32)


def packed(full, rhs, totals):
    a = full[:HALF, :HALF]
    b = full[:HALF, HALF:]
    d = full[HALF:, HALF:]
    r = lax.broadcasted_iota(jnp.int32, (HALF, HALF), 0)
    c = lax.broadcasted_iota(jnp.int32, (HALF, HALF), 1)
    both = jnp.where(r >= c, a, d)
    diag = jnp.sum(jnp.where(r == c, d, 0.0), axis=0, keepdims=True)
    extras = row_in(
        8, HALF, [(0, diag), (1, rhs[:, :HALF]), (2, rhs[:, HALF:]), (3, totals)]
    )
    return b, both, extras


def prepare(i, g, counts, pulsar, ecorr, sigma, residual, rows_s, wide_s, member_s):
    slots = counts.shape[1]
    lane = lax.broadcasted_iota(jnp.int32, (slots, HALF), 1)
    sub = lax.broadcasted_iota(jnp.int32, (slots, HALF), 0)
    count = jnp.zeros((slots, HALF), jnp.int32)
    member = jnp.zeros((slots, HALF), jnp.int32)
    amp = jnp.zeros((slots, HALF), F32)
    for s in range(slots):
        mine = pulsar[g, s]
        count = jnp.where(sub == s, counts[g, s], count)
        member = jnp.where(sub == s, mine, member)
        amp = jnp.where(sub == s, ecorr[g * PG + mine], amp)
    sig = sigma[g].astype(F32)
    res = residual[g].astype(F32)
    square = sig * sig
    valid = lane < count
    inverse = jnp.where(valid, 1.0 / square, 0.0)
    scaled = inverse * res
    total = jnp.sum(inverse, axis=1, keepdims=True)
    wsum = jnp.sum(scaled, axis=1, keepdims=True)
    jitter = amp * amp
    grown = 1.0 + jitter * total
    coef = jitter / grown
    logs = jnp.sum(jnp.where(valid, jnp.log(square), 0.0), axis=1, keepdims=True)
    rows_s[i, 0] = inverse
    rows_s[i, 1] = res
    wide_s[i, 0] = coef
    wide_s[i, 1] = coef * wsum
    member_s[i] = member
    logdet = logs + jnp.log(grown)[:, :1]
    chi = jnp.sum(scaled * res, axis=1, keepdims=True) - coef[:, :1] * wsum * wsum
    return logdet, chi


def gram_of(at_out, blocks, rows, wide, member, totals, core, acc, racc, keep, send):
    slots = blocks.shape[0]
    acc[...] = jnp.zeros_like(acc)
    racc[...] = jnp.zeros_like(racc)
    inverse_t = jnp.transpose(rows[0])
    res_t = jnp.transpose(rows[1])
    coef, pull = wide[0], wide[1]
    columns = []
    for s in range(slots):
        block = blocks[s]
        weighted = (block.astype(F32) * inverse_t[:, s : s + 1]).astype(BF)
        weighted_f = weighted.astype(F32)
        column = jnp.sum(weighted_f, axis=0, keepdims=True)
        project = jnp.sum(weighted_f * res_t[:, s : s + 1], axis=0, keepdims=True)
        mine = member[s, 0]
        acc[mine] += dot0(block, weighted)
        racc[mine, 0:1, :] += project - pull[s : s + 1, 0:1] * column
        columns.append((s, column))
    cols = row_in(slots, 2 * HALF, columns)
    head = cols.astype(BF).astype(F32)
    rest = cols - head
    left = jnp.concatenate([head, rest, head, rest], axis=0).astype(BF)
    nothing = jnp.zeros((1, HALF), F32)
    for at in range(PG):
        to = (core if at < 2 else 1 - core) * 2 + at % 2
        scale = jnp.where(member == to, coef, 0.0)
        scaled = jnp.concatenate([scale, scale], axis=1) * cols
        high = scaled.astype(BF).astype(F32)
        low = scaled - high
        right = jnp.concatenate([high, high, low, low], axis=0).astype(BF)
        full = acc[to] - dot0(left, right)
        b, both, extras = packed(
            full, racc[to, 0:1, :], totals if at % 2 == 0 else nothing
        )
        if at < 2:
            keep[at_out, at, 0:HALF, :] = b
            keep[at_out, at, HALF : 2 * HALF, :] = both
            keep[at_out, at, 2 * HALF :, :] = extras
        else:
            send[at_out, at - 2, 0:HALF, :] = b.astype(BF)
            send[at_out, at - 2, HALF : 2 * HALF, :] = both.astype(BF)
            send[at_out, at - 2, 2 * HALF :, :] = split2(extras[:4])


def first_kernel(
    counts_h, pulsar_h, ecorr_h, sigma_h, residual_h, basis,
    keep, send, later, rows_o, wide_o, member_o, totals_o,
    counts, pulsar, ecorr, sigma, residual, small_sems, buf, sems, acc, racc, rows_s, wide_s, member_s,
):
    groups = counts.shape[0]
    y = lax.axis_index("psr")
    core = lax.axis_index("c")
    small = [
        pltpu.make_async_copy(source, target, small_sems.at[k])
        for k, (source, target) in enumerate(
            (
                (counts_h, counts),
                (pulsar_h, pulsar),
                (ecorr_h, ecorr),
                (sigma_h, sigma),
                (residual_h, residual),
            )
        )
    ]
    copies = []
    for k, i in enumerate(ORDER):
        target = buf if k == 0 else later.at[k - 1]
        copies.append(pltpu.make_async_copy(basis.at[lax.rem(y + i, groups)], target, sems.at[k]))
    copies[0].start()
    for copy in small:
        copy.start()
    for copy in copies[1:]:
        copy.start()
    for copy in small:
        copy.wait()
    logdet, chi = 0.0, 0.0
    for k, i in enumerate(ORDER):
        places = (rows_s, wide_s, member_s, 0) if k == 0 else (rows_o, wide_o, member_o, k - 1)
        g = lax.rem(y + i, groups)
        part = prepare(places[3], g, counts, pulsar, ecorr, sigma, residual, *places[:3])
        logdet, chi = logdet + part[0], chi + part[1]
    lane1 = lax.broadcasted_iota(jnp.int32, (1, HALF), 1)
    totals = jnp.where(
        lane1 == 0,
        jnp.sum(logdet, axis=0, keepdims=True),
        jnp.where(lane1 == 1, jnp.sum(chi, axis=0, keepdims=True), 0.0),
    )
    totals_o[...] = jnp.broadcast_to(totals, totals_o.shape)
    copies[0].wait()
    gram_of(0, buf, rows_s[0], wide_s[0], member_s[0], totals, core, acc, racc, keep, send)
    for copy in copies[1:]:
        copy.wait()


def later_kernel(which, later, rows, wide, member, totals, after, keep, send, acc, racc):
    core = lax.axis_index("c")
    for k, i in enumerate(which):
        gram_of(
            k, later.at[i], rows[i], wide[i], member[i], totals[0:1], core, acc, racc, keep, send
        )


def packs(n):
    return [((n, 2, 2 * HALF + 8, HALF), F32), ((n, 2, 2 * HALF + 8, HALF), BF)]


def accumulators(width):
    return [pltpu.VMEM((PG, width, width), F32), pltpu.VMEM((PG, 8, width), F32)]


def first_terms(basis, residual, sigma, counts, pulsar, ecorr):
    groups, slots, rows, width = basis.shape
    operands = (counts, pulsar, ecorr, sigma, residual, basis)
    return call(
        first_kernel,
        packs(1)
        + [
            ((groups - 1, slots, rows, width), BF),
            ((groups - 1, 2, slots, rows), F32),
            ((groups - 1, 2, slots, rows), F32),
            ((groups - 1, slots, rows), jnp.int32),
            ((8, HALF), F32),
        ],
        [
            pltpu.SMEM((groups, slots), jnp.int32),
            pltpu.SMEM((groups, slots), jnp.int32),
            pltpu.SMEM(ecorr.shape, F32),
            pltpu.VMEM((groups, slots, rows), BF),
            pltpu.VMEM((groups, slots, rows), BF),
            pltpu.SemaphoreType.DMA((5,)),
            pltpu.VMEM((slots, rows, width), BF),
            pltpu.SemaphoreType.DMA((groups,)),
            *accumulators(width),
            pltpu.VMEM((1, 2, slots, rows), F32),
            pltpu.VMEM((1, 2, slots, rows), F32),
            pltpu.VMEM((1, slots, rows), jnp.int32),
        ],
        [pltpu.with_memory_space_constraint(a, pltpu.HBM) for a in operands],
        in_specs=[pl.BlockSpec(memory_space=pltpu.HBM)] * 6,
    )


def later_terms(which, shared, after):
    vmem = pl.BlockSpec(memory_space=pltpu.VMEM)
    return call(
        functools.partial(later_kernel, which),
        packs(len(which)),
        accumulators(shared[0].shape[-1]),
        (*shared, after),
        in_specs=[vmem] * len(shared) + [pl.BlockSpec(memory_space=pl.ANY)],
        flops=len(which) * 10**9,
    )


def cores_kernel(at, relayed, keep, got, *refs):
    extra = refs[0] if relayed is not None else None
    for j in range(2):
        body = keep[at, j, : 2 * HALF] + got[at, j, : 2 * HALF].astype(F32)
        extras = keep[at, j, 2 * HALF : 2 * HALF + 4] + joined2(got[at, j, 2 * HALF :])
        if relayed == j:
            body = body + extra[: 2 * HALF].astype(F32)
            extras = extras + joined2(extra[2 * HALF :])
        out = refs[j] if relayed is None else refs[1].at[j]
        out[: 2 * HALF] = body.astype(BF)
        out[2 * HALF :] = split2(extras)


def own_spots():
    r = lax.broadcasted_iota(jnp.int32, (HALF, HALF), 0)
    c = lax.broadcasted_iota(jnp.int32, (HALF, HALF), 1)
    inside = (r // 4 == c // 4) & (r < c)
    r, c = r % 4, c % 4
    return (
        inside & (r == 0),
        inside & (r == 1) & (c == 2),
        inside & (r == 1) & (c == 3),
        inside & (r == 2),
    )


def with_extras(square, spots, before, after, head, rest):
    for spot, value in zip(spots, (before, after, head, rest)):
        square = jnp.where(spot, jnp.broadcast_to(value, square.shape), square)
    return square


def unpack_kernel(at, keep, got, *refs):
    arrived, out, full = refs[:-2], refs[-2], refs[-1]
    r = lax.broadcasted_iota(jnp.int32, (HALF, HALF), 0)
    c = lax.broadcasted_iota(jnp.int32, (HALF, HALF), 1)
    spots = own_spots()
    for j in range(2):
        body = keep[at, j, : 2 * HALF] + got[at, j, : 2 * HALF].astype(F32)
        extras = keep[at, j, 2 * HALF : 2 * HALF + 4] + joined2(got[at, j, 2 * HALF :])
        for a in arrived:
            body = body + a[j, : 2 * HALF].astype(F32)
            extras = extras + joined2(a[j, 2 * HALF :])
        b, both = body[:HALF], body[HALF:]
        flipped = jnp.transpose(both)
        if j == 0:
            totals = extras[3:4]
        value = totals[:, j : j + 1]
        head = value.astype(BF).astype(F32)
        before = jnp.roll(extras[1:3], 1, axis=1)
        after = jnp.roll(extras[1:3], HALF - 1, axis=1)
        low = jnp.where(r >= c, both, flipped)
        high = jnp.where(
            r < c, both, jnp.where(r > c, flipped, jnp.broadcast_to(extras[0:1], (HALF, HALF)))
        )
        full[j, :HALF, :HALF] = with_extras(
            low, spots, before[0:1], after[0:1], head, value - head
        )
        full[j, :HALF, HALF:] = b
        full[j, HALF:, :HALF] = jnp.transpose(b)
        full[j, HALF:, HALF:] = with_extras(
            high, spots, before[1:2], after[1:2], head, value - head
        )
    sub = lax.broadcasted_iota(jnp.int32, (8, 2 * HALF), 0)
    n_x, n_z = lax.axis_size("x"), lax.axis_size("z")
    for m in range(n_z * n_x):
        to = 2 * ((m % n_x) * n_z + m // n_x)
        t0, t1 = full[0, 8 * m : 8 * m + 8], full[1, 8 * m : 8 * m + 8]
        out[to] = jnp.where(sub < 4, t0, jnp.roll(t1, 4, axis=0)).astype(BF)
        out[to + 1] = jnp.where(sub < 4, jnp.roll(t0, 4, axis=0), t1).astype(BF)


def final_kernel(norm, every, arrived, gram, rhs, totals):
    at = 8 * lax.axis_index("z") + 2 * lax.axis_index("x") + lax.axis_index("c")
    sides = []
    for core in range(2):
        side = arrived[core].astype(F32)
        for k in range(1, arrived.shape[0] // 2):
            side = side + arrived[2 * k + core].astype(F32)
        sides.append(side)
    block = jnp.concatenate(sides, axis=0)
    shape = block.shape
    lane = lax.broadcasted_iota(jnp.int32, shape, 1)
    sub = lax.rem(lax.broadcasted_iota(jnp.int32, shape, 0), 4)
    wide = [
        jnp.broadcast_to(
            jnp.sum(jnp.where(lane == 4 * at + k, block, 0.0), axis=1, keepdims=True), shape
        )
        for k in range(4)
    ]
    out = block
    for r in range(4):
        for c in range(r + 1, 4):
            mirror = jnp.roll(wide[r], r - c, axis=0)
            out = jnp.where((sub == r) & (lane == 4 * at + c), mirror, out)
    out = out * (1.0 / norm)
    spread = jnp.where(
        lane == 0,
        wide[1],
        jnp.where(lane == 1, wide[2], jnp.where(lane == 2, wide[3], jnp.roll(wide[2], -1, axis=0))),
    )
    spread = spread * (1.0 / norm)
    for q in range(PG):
        gram[q] = out[4 * q : 4 * q + 4]
        rhs[q : q + 1, :] = spread[4 * q : 4 * q + 1, 0:4]
    for k in range(2):
        totals[k] = (wide[3][4 * k + 1, 0] + wide[3][4 * k + 2, 0]) * (1.0 / every)


def call(kernel, outs, scratch, operands, out_specs=None, in_specs=None, flops=None):
    vmem = pl.BlockSpec(memory_space=pltpu.VMEM)
    cost = None
    if flops:
        cost = pl.CostEstimate(flops=flops, bytes_accessed=0, transcendentals=0)
    return pl.pallas_call(
        kernel,
        out_shape=tuple(jax.ShapeDtypeStruct(s, d) for s, d in outs),
        in_specs=in_specs or [vmem] * len(operands),
        out_specs=out_specs or tuple([vmem] * len(outs)),
        scratch_shapes=scratch,
        cost_estimate=cost,
        compiler_params=pltpu.CompilerParams(vmem_limit_bytes=GRANT),
    )(*operands)


def swapped(value, axis, by):
    return lax.ppermute(value, axis, [(k, k ^ by) for k in range(lax.axis_size(axis))])


def shifted(value, axis, by):
    n = lax.axis_size(axis)
    return lax.ppermute(value, axis, [(k, (k + by) % n) for k in range(n)])


def across_cores(at, keep, got, relayed=None, extra=None):
    wire = (2 * HALF + 8, HALF)
    outs = [(wire, BF)] * 2 if relayed is None else [((2, *wire), BF)]
    operands = (keep, got) if relayed is None else (keep, got, extra)
    return call(functools.partial(cores_kernel, at, relayed), outs, [], operands)


def reduced(basis, residual, sigma, counts, pulsar, ecorr):
    groups = lax.axis_size("psr")
    slots, rows, width = basis.shape[2:]
    ndp = lax.axis_size(("z", "x", "c"))
    norm = float(ndp * slots * rows)
    every = norm * groups * groups
    keep, send, *shared = first_terms(
        basis[0], residual[0], sigma[0], counts[0], pulsar[0], ecorr
    )
    got = swapped(send, "c", 1)
    keep_b, send_b = later_terms((0,), shared, shared[-1])
    up, down = across_cores(0, keep, got)
    from_below = shifted(up, "psr", 1)
    from_above = shifted(down, "psr", -1)
    got_b = swapped(send_b, "c", 1)
    keep_c, send_c = later_terms((1,), shared, up)
    got_c = swapped(send_c, "c", 1)
    keep, send = later_terms((2,), shared, keep_c)
    got = swapped(send, "c", 1)
    (mine,) = across_cores(0, keep_b, got_b, 0, from_below)
    arrived = [shifted(mine, "psr", 1)]
    (mine,) = across_cores(0, keep_c, got_c, 1, from_above)
    arrived.append(shifted(mine, "psr", -1))
    (wire,) = call(
        functools.partial(unpack_kernel, 0),
        [((ndp, 8, width), BF)],
        [pltpu.VMEM((2, width, width), F32)],
        (keep, got, *arrived),
    )
    wire = lax.all_to_all(wire, ("x", "z", "c"), 0, 0, tiled=True)
    return call(
        functools.partial(final_kernel, norm, every),
        [((PG, width // ndp, width), F32), ((PG, width // ndp), F32), ((2,), F32)],
        [],
        (wire,),
        (
            pl.BlockSpec(memory_space=pltpu.VMEM),
            pl.BlockSpec(memory_space=pltpu.VMEM),
            pl.BlockSpec(memory_space=pltpu.SMEM),
        ),
    )


def solution(mesh):
    finer = Mesh(mesh.devices.reshape(8, 4, 2, mesh.shape["psr"]), AXES)
    in_specs = (
        P(AXES, None, None, None, None),
        P(AXES, None, None, None),
        P(AXES, None, None, None),
        P(AXES, None, None),
        P(AXES, None, None),
        P(),
    )
    out_specs = (P("psr", ("z", "x", "c"), None), P("psr", ("z", "x", "c")), P())
    return jax.shard_map(
        reduced, mesh=finer, in_specs=in_specs, out_specs=out_specs, check_vma=False
    )
```
